32 devices in a mesh: zero: 4 (over z), width: 4 (over y, x), unit: 2 (over core).
Axes of the slice: x: 2, y: 2, z: 4, core: 2. Of those that a mesh axis runs over, the one named last changes fastest.
Arguments:
- grad_stack: float32 [64, 128, 2048], P('unit', 'zero', 'width'), parts along dimension 0, may hold values from -6 to 6
- moment_stack: float32 [64, 128, 2048], P('unit', 'zero', 'width'), parts along dimension 0, may hold values from -6 to 6
- weight_stack: float32 [64, 128, 2048], P('unit', 'zero', 'width'), parts along dimension 0, may hold values from -0.1875 to 0.1875
Outputs:
- new_weights: float32 [64, 128, 2048], P('unit', 'zero', 'width'), parts along dimension 0
- new_momentum: float32 [64, 128, 2048], P('unit', 'zero', 'width'), parts along dimension 0
The draws below stay inside these ranges and needn't reach their ends.
There are 2 independent parts, one for each index of `unit`. The reference program is written for one: setup_inputs(seed, part) draws one part's arguments, and reference() takes and returns one part's arrays. A program takes and returns all parts, laid end to end along the dimension named above; each array names one. Nothing has to cross between parts.
All inputs are finite; a program needn't handle non-finite values.
Results may differ from the reference program's by a relative error of at most 0.0001.
Values sent between devices are 32-bit elements; how exact they have to be, the bound alone decides.
A program may use at most 64 MiB of HBM per device.

```python
import jax
import jax.numpy as jnp
from jax import lax

SIDE = 128
WIDE = 2048
MATS = 32
ITERS = 3


def shard_levels(key, dims, shards, least, top_value):
    def one(dim, parts):
        steps = jax.random.uniform(jax.random.fold_in(jax.random.fold_in(key, 6), dim), (parts,), jnp.float32, least / len(shards), top_value / len(shards))
        return jnp.repeat(jnp.exp(steps), dims[dim] // parts).reshape((-1,) + (1,) * (len(dims) - dim - 1))

    loudness = one(*shards[0])
    for cut in shards[1:]:
        loudness = loudness * one(*cut)
    return loudness


def noise(key, shape, width, most, cuts=(), held_as=jnp.bfloat16):
    entries = width * jax.random.normal(key, shape, jnp.float32)
    if cuts:
        entries = entries * shard_levels(key, shape, cuts, -0.22, 0.18)
    return jnp.clip(entries, -most, most).astype(held_as)


def setup_inputs(seed: int = 0, part: int = 0) -> dict:
    splits = jax.random.split(jax.random.key(seed), 4)
    own_keys = jax.random.split(jax.random.fold_in(splits[3], part), 4)
    return {
        "grad_stack": noise(own_keys[0], (MATS, SIDE, WIDE), 1.0, 6.0, ((1, 4), (2, 4)), jnp.float32),
        "moment_stack": noise(own_keys[1], (MATS, SIDE, WIDE), 1.0, 6.0, ((1, 4), (2, 4)), jnp.float32),
        "weight_stack": noise(own_keys[2], (MATS, SIDE, WIDE), 0.03, 0.1875, ((1, 4), (2, 4)), jnp.float32),
    }


hold_rate = 0.95
learn_rate = 0.8
decay_rate = 0.1

def reference(grad_stack, moment_stack, weight_stack):
    new_momentum = hold_rate * moment_stack + grad_stack

    def orthogonal_one(stack):
        iterate = stack[None]
        iterate = iterate * lax.rsqrt(lax.optimization_barrier(jnp.sum(iterate * iterate, axis=(1, 2), keepdims=True)) + 1e-06)
        for step in range(ITERS):
            gram = jnp.einsum('mik,mjk->mij', iterate, iterate, precision=lax.Precision.HIGHEST)
            mixed = -4.775 * gram + 2.0315 * jnp.einsum('mij,mjk->mik', gram, gram, precision=lax.Precision.HIGHEST)
            iterate = 3.4445 * iterate + jnp.einsum('mij,mjk->mik', mixed, iterate, precision=lax.Precision.HIGHEST)
        return iterate[0]
    iterate = lax.map(orthogonal_one, new_momentum)
    new_weights = (1.0 - learn_rate * decay_rate) * weight_stack - learn_rate * iterate
    return (new_weights, new_momentum)
```

```python
import functools

import jax
import jax.numpy as jnp
from jax import lax
from jax.experimental import pallas as pl
from jax.experimental.pallas import tpu as pltpu
from jax.sharding import PartitionSpec as P

ITERS = 3
GATHER_FROM = 1
RESULT_FROM = 1
CHUNKS = (4, 2, 1)
MESH = pl.DeviceIdType.MESH


hold_rate = 0.95
learn_rate = 0.8
decay_rate = 0.1
keep_rate = 1.0 - learn_rate * decay_rate


def split(value):
    high = value.astype(jnp.bfloat16)
    low = (value - high.astype(jnp.float32)).astype(jnp.bfloat16)
    return high, low


def product(left, right, over):
    dims = (((1,), (over,)), ((), ()))
    dot = functools.partial(lax.dot_general, dimension_numbers=dims, preferred_element_type=jnp.float32)
    (lh, ll), (rh, rl) = left, right
    return dot(lh, rh) + (dot(lh, rl) + dot(ll, rh))


def orders(count):
    near = list(range(1, count))
    return near[GATHER_FROM:] + near[:GATHER_FROM], near[RESULT_FROM:] + near[:RESULT_FROM]


def paired(index, d, count):
    if d == 0:
        return index
    out, bit = 0, 1
    while bit < count:
        out = out + bit * ((index // bit + d // bit) % 2)
        bit *= 2
    return out


def factor(gram):
    side = gram.shape[0]
    rows = lax.broadcasted_iota(jnp.int32, (side, side), 0)
    cols = lax.broadcasted_iota(jnp.int32, (side, side), 1)
    eye = jnp.where(rows == cols, 1.0, 0.0).astype(jnp.float32)
    total = jnp.sum(jnp.sum(gram * eye, axis=1, keepdims=True), axis=0, keepdims=True)
    scale = lax.rsqrt(total + 1e-06)
    gram = gram * (scale * scale)
    held = None
    for step in range(ITERS):
        gs = split(gram)
        mixed = 3.4445 * eye - 4.775 * gram + 2.0315 * product(gs, gs, 0)
        ms = split(mixed)
        held = mixed if held is None else product(ms, split(held), 0)
        if step < ITERS - 1:
            gram = product(split(product(ms, gs, 0)), ms, 0)
    return held * scale


def kernel(nz, nw, chunks, per, grad, moment, weight, new_weights, new_momentum,
           grads, moments, weights, gather, grams, result, back,
           l_sem, w_sem, g_send, g_recv, p_send, p_recv, r_send, r_recv):
    zi, wi = lax.axis_index("zero"), lax.axis_index("width")
    mats = chunks * per
    rows, cols = grad.shape[1], grad.shape[2]
    side = nz * rows
    gather_order, result_order = orders(nz)
    pieces = [(d, k) for k in range(chunks) for d in gather_order + [0]]

    def partner(d):
        return paired(zi, d, nz)

    barrier = pltpu.get_barrier_semaphore()
    for d in range(1, nz):
        pl.semaphore_signal(barrier, inc=1, device_id={"zero": partner(d)}, device_id_type=MESH)
    for d in range(1, nw):
        pl.semaphore_signal(barrier, inc=1, device_id={"width": lax.rem(wi + d, nw)}, device_id_type=MESH)

    def piece(d, k):
        return pl.ds(partner(d) * mats + k * per, per)

    def group(n):
        return 0 if n == 0 else 1 + n // nz

    def load(which, n):
        source, target = ((grad, grads), (moment, moments))[which]
        return pltpu.make_async_copy(source.at[piece(*pieces[n])], target.at[piece(*pieces[n])], l_sem.at[group(n)])

    def load_weight():
        return pltpu.make_async_copy(weight, weights, w_sem.at[0])

    def wait_all(sem, *refs):
        for ref in refs:
            pltpu.make_async_copy(ref, ref, sem).wait()

    def gather_copy(d, k):
        return pltpu.make_async_remote_copy(
            src_ref=new_momentum.at[piece(d, k)],
            dst_ref=gather.at[zi, pl.ds(k * per, per)],
            send_sem=g_send.at[0], recv_sem=g_recv.at[k],
            device_id={"zero": partner(d)}, device_id_type=MESH)

    def gram_copy(d, k):
        return pltpu.make_async_remote_copy(
            src_ref=grams.at[wi, pl.ds(k * per, per)],
            dst_ref=grams.at[wi, pl.ds(k * per, per)],
            send_sem=p_send.at[0], recv_sem=p_recv.at[k],
            device_id={"width": lax.rem(wi + d, nw)}, device_id_type=MESH)

    def result_copy(d, k):
        return pltpu.make_async_remote_copy(
            src_ref=result.at[partner(d), pl.ds(k * per, per)],
            dst_ref=back.at[piece(0, k)],
            send_sem=r_send.at[0], recv_sem=r_recv.at[k],
            device_id={"zero": partner(d)}, device_id_type=MESH)

    for n in range(len(pieces)):
        load(0, n).start()
        load(1, n).start()

    def momentum(n):
        d, k = pieces[n]
        if n == 0 or group(n) != group(n - 1):
            members = sum(group(m) == group(n) for m in range(len(pieces)))
            wait_all(l_sem.at[group(n)], grads.at[pl.ds(0, 2 * members * per)])
        value = hold_rate * moments[piece(d, k)] + grads[piece(d, k)]
        new_momentum[piece(d, k)] = value
        if d == 0:
            gather[zi, pl.ds(k * per, per)] = value

    def release(d, k):
        if d:
            gather_copy(d, k).start()

    for n in range(len(pieces)):
        momentum(n)
        if n == 1:
            pl.semaphore_wait(barrier, nz + nw - 2)
        if n:
            release(*pieces[n - 1])
    release(*pieces[-1])
    load_weight().start()

    def whole(i):
        return split(gather[:, i].reshape(side, cols))

    def finish(k):
        wait_all(p_recv.at[k], grams.at[pl.ds(0, nw - 1), pl.ds(k * per, per)])

        def one(j, carry):
            i = k * per + j
            gram = grams[0, i]
            for w in range(1, nw):
                gram = gram + grams[w, i]
            out = product(split(factor(gram)), whole(i), 0)
            result[:, i] = out.reshape(nz, rows, cols)
            return carry

        lax.fori_loop(0, per, one, 0)
        for d in result_order:
            result_copy(d, k).start()

    for k in range(chunks):
        wait_all(g_recv.at[k], gather.at[pl.ds(0, nz - 1), pl.ds(k * per, per)])

        def make(j, carry):
            i = k * per + j
            x = whole(i)
            grams[wi, i] = product(x, x, 1)
            return carry

        lax.fori_loop(0, per, make, 0)
        for d in range(1, nw):
            gram_copy(d, k).start()
        finish(k)

    load_weight().wait()
    for k in range(chunks):
        new_weights[piece(0, k)] = keep_rate * weights[piece(0, k)] - learn_rate * result[zi, pl.ds(k * per, per)]
    for k in range(chunks):
        wait_all(r_recv.at[k], back.at[pl.ds(0, (nz - 1) * per)])
        for d in result_order:
            new_weights[piece(d, k)] = keep_rate * weights[piece(d, k)] - learn_rate * back[piece(d, k)]

    wait_all(g_send.at[0], gather.at[pl.ds(0, nz - 1)])
    wait_all(p_send.at[0], grams.at[pl.ds(0, nw - 1)])
    wait_all(r_send.at[0], result.at[pl.ds(0, nz - 1)])


def by_kernel(nz, nw, grad, moment, weight):
    total, rows, cols = grad.shape
    side, mats = nz * rows, total // nz
    chunks = next(c for c in CHUNKS if mats % c == 0)
    dma = pltpu.SemaphoreType.DMA
    anywhere = pl.BlockSpec(memory_space=pl.ANY)
    shape = pltpu.VMEM(grad.shape, jnp.float32)
    local = pltpu.VMEM((total, rows, cols), jnp.float32)
    shared = pltpu.VMEM((nz, mats, rows, cols), jnp.float32)
    return pl.pallas_call(
        functools.partial(kernel, nz, nw, chunks, mats // chunks),
        out_shape=(shape, shape),
        in_specs=[anywhere] * 3,
        out_specs=(pl.BlockSpec(memory_space=pltpu.VMEM),) * 2,
        scratch_shapes=[
            local, local, local,
            shared,
            pltpu.VMEM((nw, mats, side, side), jnp.float32),
            shared,
            local,
            dma((chunks + 1,)), dma((1,)),
            dma((1,)), dma((chunks,)),
            dma((1,)), dma((chunks,)),
            dma((1,)), dma((chunks,)),
        ],
        compiler_params=pltpu.CompilerParams(
            collective_id=0, has_side_effects=True, vmem_limit_bytes=40 * 2**20),
    )(*(pltpu.with_memory_space_constraint(x, pltpu.HBM) for x in (grad, moment, weight)))


def by_ops(new_momentum):
    moved = lax.all_to_all(new_momentum, "zero", split_axis=0, concat_axis=1, tiled=True)
    gram = jnp.einsum("mik,mjk->mij", moved, moved, precision=lax.Precision.HIGHEST)
    gram = lax.psum(gram, "width")
    eye = jnp.eye(gram.shape[1], dtype=jnp.float32)
    scale = lax.rsqrt(jnp.sum(gram * eye, axis=(1, 2), keepdims=True) + 1e-06)
    gram = gram * (scale * scale)
    dot = functools.partial(jnp.einsum, "mij,mjk->mik", precision=lax.Precision.HIGHEST)
    held = None
    for step in range(ITERS):
        mixed = 3.4445 * eye - 4.775 * gram + 2.0315 * dot(gram, gram)
        held = mixed if held is None else dot(mixed, held)
        gram = dot(dot(mixed, gram), mixed)
    out = dot(held * scale, moved)
    return lax.all_to_all(out, "zero", split_axis=1, concat_axis=0, tiled=True)


def body(nz, nw, grad_stack, moment_stack, weight_stack):
    if grad_stack.shape[1] % 8 == 0 and nz & (nz - 1) == 0:
        return by_kernel(nz, nw, grad_stack, moment_stack, weight_stack)
    new_momentum = hold_rate * moment_stack + grad_stack
    new_weights = keep_rate * weight_stack - learn_rate * by_ops(new_momentum)
    return (new_weights, new_momentum)


def solution(mesh):
    return jax.shard_map(
        functools.partial(body, mesh.shape["zero"], mesh.shape["width"]),
        mesh=mesh,
        in_specs=(
            P("unit", "zero", "width"),
            P("unit", "zero", "width"),
            P("unit", "zero", "width"),
        ),
        out_specs=(P("unit", "zero", "width"), P("unit", "zero", "width")),
        check_vma=False,
    )
```

```python
import functools

import jax
import jax.numpy as jnp
from jax import lax
from jax.experimental import pallas as pl
from jax.experimental.pallas import tpu as pltpu
from jax.sharding import PartitionSpec as P

ITERS = 3
GATHER_FROM = 1
RESULT_FROM = 1
CHUNKS = (4, 2, 1)
PARTS = (8, 4, 2, 1)
MESH = pl.DeviceIdType.MESH


hold_rate = 0.95
learn_rate = 0.8
decay_rate = 0.1
keep_rate = 1.0 - learn_rate * decay_rate


def split(value):
    high = value.astype(jnp.bfloat16)
    low = (value - high.astype(jnp.float32)).astype(jnp.bfloat16)
    return high, low


def product(left, right, over):
    dims = (((1,), (over,)), ((), ()))
    dot = functools.partial(lax.dot_general, dimension_numbers=dims, preferred_element_type=jnp.float32)
    (lh, ll), (rh, rl) = left, right
    return dot(lh, rh) + (dot(lh, rl) + dot(ll, rh))


def orders(count):
    near = list(range(1, count))
    return near[GATHER_FROM:] + near[:GATHER_FROM], near[RESULT_FROM:] + near[:RESULT_FROM]


def paired(index, d, count):
    if d == 0:
        return index
    out, bit = 0, 1
    while bit < count:
        out = out + bit * ((index // bit + d // bit) % 2)
        bit *= 2
    return out


def factor(gram):
    side = gram.shape[0]
    rows = lax.broadcasted_iota(jnp.int32, (side, side), 0)
    cols = lax.broadcasted_iota(jnp.int32, (side, side), 1)
    eye = jnp.where(rows == cols, 1.0, 0.0).astype(jnp.float32)
    total = jnp.sum(jnp.sum(gram * eye, axis=1, keepdims=True), axis=0, keepdims=True)
    scale = lax.rsqrt(total + 1e-06)
    gram = gram * (scale * scale)
    held = None
    for step in range(ITERS):
        gs = split(gram)
        mixed = 3.4445 * eye - 4.775 * gram + 2.0315 * product(gs, gs, 0)
        ms = split(mixed)
        held = mixed if held is None else product(ms, split(held), 0)
        if step < ITERS - 1:
            gram = product(split(product(ms, gs, 0)), ms, 0)
    return held * scale


def kernel(nz, nw, chunks, per, grad, moment, weight, new_weights, new_momentum,
           grads, moments, weights, gather, grams, result, back,
           l_sem, w_sem, g_send, g_recv, p_send, p_recv, r_send, r_recv):
    zi, wi = lax.axis_index("zero"), lax.axis_index("width")
    mats = chunks * per
    rows, cols = grad.shape[1], grad.shape[2]
    side = nz * rows
    gather_order, result_order = orders(nz)
    pieces = [(d, k) for k in range(chunks) for d in gather_order + [0]]

    def partner(d):
        return paired(zi, d, nz)

    barrier = pltpu.get_barrier_semaphore()
    for d in range(1, nz):
        pl.semaphore_signal(barrier, inc=1, device_id={"zero": partner(d)}, device_id_type=MESH)
    for d in range(1, nw):
        pl.semaphore_signal(barrier, inc=1, device_id={"width": lax.rem(wi + d, nw)}, device_id_type=MESH)

    def piece(d, k):
        return pl.ds(partner(d) * mats + k * per, per)

    def group(n):
        return 0 if n == 0 else 1 + n // nz

    def load(which, n):
        source, target = ((grad, grads), (moment, moments))[which]
        return pltpu.make_async_copy(source.at[piece(*pieces[n])], target.at[piece(*pieces[n])], l_sem.at[group(n)])

    def load_weight():
        return pltpu.make_async_copy(weight, weights, w_sem.at[0])

    def wait_all(sem, *refs):
        for ref in refs:
            pltpu.make_async_copy(ref, ref, sem).wait()

    def gather_copy(d, k):
        return pltpu.make_async_remote_copy(
            src_ref=new_momentum.at[piece(d, k)],
            dst_ref=gather.at[zi, pl.ds(k * per, per)],
            send_sem=g_send.at[0], recv_sem=g_recv.at[k],
            device_id={"zero": partner(d)}, device_id_type=MESH)

    def gram_copy(d, k):
        return pltpu.make_async_remote_copy(
            src_ref=grams.at[wi, pl.ds(k * per, per)],
            dst_ref=grams.at[wi, pl.ds(k * per, per)],
            send_sem=p_send.at[0], recv_sem=p_recv.at[k],
            device_id={"width": lax.rem(wi + d, nw)}, device_id_type=MESH)

    def result_copy(d, k):
        return pltpu.make_async_remote_copy(
            src_ref=result.at[partner(d), pl.ds(k * per, per)],
            dst_ref=back.at[piece(0, k)],
            send_sem=r_send.at[0], recv_sem=r_recv.at[k],
            device_id={"zero": partner(d)}, device_id_type=MESH)

    for n in range(len(pieces)):
        load(0, n).start()
        load(1, n).start()

    def momentum(n):
        d, k = pieces[n]
        if n == 0 or group(n) != group(n - 1):
            members = sum(group(m) == group(n) for m in range(len(pieces)))
            wait_all(l_sem.at[group(n)], grads.at[pl.ds(0, 2 * members * per)])
        value = hold_rate * moments[piece(d, k)] + grads[piece(d, k)]
        new_momentum[piece(d, k)] = value
        if d == 0:
            gather[zi, pl.ds(k * per, per)] = value

    def release(d, k):
        if d:
            gather_copy(d, k).start()

    for n in range(len(pieces)):
        momentum(n)
        if n == 1:
            pl.semaphore_wait(barrier, nz + nw - 2)
        if n:
            release(*pieces[n - 1])
    release(*pieces[-1])
    load_weight().start()

    def whole(i):
        return split(gather[:, i].reshape(side, cols))

    def finish(k):
        wait_all(p_recv.at[k], grams.at[pl.ds(0, nw - 1), pl.ds(k * per, per)])

        def one(j, carry):
            i = k * per + j
            gram = grams[0, i]
            for w in range(1, nw):
                gram = gram + grams[w, i]
            out = product(split(factor(gram)), whole(i), 0)
            result[:, i] = out.reshape(nz, rows, cols)
            return carry

        lax.fori_loop(0, per, one, 0)
        for d in result_order:
            result_copy(d, k).start()

    for k in range(chunks):
        wait_all(g_recv.at[k], gather.at[pl.ds(0, nz - 1), pl.ds(k * per, per)])

        def make(j, carry):
            i = k * per + j
            x = whole(i)
            grams[wi, i] = product(x, x, 1)
            return carry

        lax.fori_loop(0, per, make, 0)
        for d in range(1, nw):
            gram_copy(d, k).start()
        finish(k)

    load_weight().wait()
    for k in range(chunks):
        new_weights[piece(0, k)] = keep_rate * weights[piece(0, k)] - learn_rate * result[zi, pl.ds(k * per, per)]
    for k in range(chunks):
        wait_all(r_recv.at[k], back.at[pl.ds(0, (nz - 1) * per)])
        for d in result_order:
            new_weights[piece(d, k)] = keep_rate * weights[piece(d, k)] - learn_rate * back[piece(d, k)]

    wait_all(g_send.at[0], gather.at[pl.ds(0, nz - 1)])
    wait_all(p_send.at[0], grams.at[pl.ds(0, nw - 1)])
    wait_all(r_send.at[0], result.at[pl.ds(0, nz - 1)])


def store(*refs):
    count = len(refs) // 2
    sem = refs[-1]
    length = refs[0].shape[0]
    parts = next(p for p in PARTS if length % p == 0)
    for p in range(parts):
        part = pl.ds(p * length // parts, length // parts)
        for n in range(count):
            pltpu.make_async_copy(refs[n].at[part], refs[count + n].at[part], sem.at[n]).start()
    for n in range(count):
        pltpu.make_async_copy(refs[n], refs[count + n], sem.at[n]).wait()


def stored(*arrays):
    inside = pl.BlockSpec(memory_space=pltpu.VMEM)
    return pl.pallas_call(
        store,
        out_shape=tuple(pltpu.HBM(x.shape, x.dtype) for x in arrays),
        in_specs=[inside] * len(arrays),
        out_specs=(pl.BlockSpec(memory_space=pltpu.HBM),) * len(arrays),
        scratch_shapes=[pltpu.SemaphoreType.DMA((len(arrays),))],
        compiler_params=pltpu.CompilerParams(vmem_limit_bytes=2**20),
    )(*(pltpu.with_memory_space_constraint(x, pltpu.VMEM) for x in arrays))


def by_kernel(nz, nw, grad, moment, weight):
    total, rows, cols = grad.shape
    side, mats = nz * rows, total // nz
    chunks = next(c for c in CHUNKS if mats % c == 0)
    dma = pltpu.SemaphoreType.DMA
    anywhere = pl.BlockSpec(memory_space=pl.ANY)
    shape = pltpu.VMEM(grad.shape, jnp.float32)
    local = pltpu.VMEM((total, rows, cols), jnp.float32)
    shared = pltpu.VMEM((nz, mats, rows, cols), jnp.float32)
    results = pl.pallas_call(
        functools.partial(kernel, nz, nw, chunks, mats // chunks),
        out_shape=(shape, shape),
        in_specs=[anywhere] * 3,
        out_specs=(pl.BlockSpec(memory_space=pltpu.VMEM),) * 2,
        scratch_shapes=[
            local, local, local,
            shared,
            pltpu.VMEM((nw, mats, side, side), jnp.float32),
            shared,
            local,
            dma((chunks + 1,)), dma((1,)),
            dma((1,)), dma((chunks,)),
            dma((1,)), dma((chunks,)),
            dma((1,)), dma((chunks,)),
        ],
        compiler_params=pltpu.CompilerParams(
            collective_id=0, has_side_effects=True, vmem_limit_bytes=40 * 2**20),
    )(*(pltpu.with_memory_space_constraint(x, pltpu.HBM) for x in (grad, moment, weight)))
    return stored(*results)


def by_ops(new_momentum):
    moved = lax.all_to_all(new_momentum, "zero", split_axis=0, concat_axis=1, tiled=True)
    gram = jnp.einsum("mik,mjk->mij", moved, moved, precision=lax.Precision.HIGHEST)
    gram = lax.psum(gram, "width")
    eye = jnp.eye(gram.shape[1], dtype=jnp.float32)
    scale = lax.rsqrt(jnp.sum(gram * eye, axis=(1, 2), keepdims=True) + 1e-06)
    gram = gram * (scale * scale)
    dot = functools.partial(jnp.einsum, "mij,mjk->mik", precision=lax.Precision.HIGHEST)
    held = None
    for step in range(ITERS):
        mixed = 3.4445 * eye - 4.775 * gram + 2.0315 * dot(gram, gram)
        held = mixed if held is None else dot(mixed, held)
        gram = dot(dot(mixed, gram), mixed)
    out = dot(held * scale, moved)
    return lax.all_to_all(out, "zero", split_axis=1, concat_axis=0, tiled=True)


def body(nz, nw, grad_stack, moment_stack, weight_stack):
    if grad_stack.shape[1] % 8 == 0 and nz & (nz - 1) == 0:
        return by_kernel(nz, nw, grad_stack, moment_stack, weight_stack)
    new_momentum = hold_rate * moment_stack + grad_stack
    new_weights = keep_rate * weight_stack - learn_rate * by_ops(new_momentum)
    return (new_weights, new_momentum)


def solution(mesh):
    return jax.shard_map(
        functools.partial(body, mesh.shape["zero"], mesh.shape["width"]),
        mesh=mesh,
        in_specs=(
            P("unit", "zero", "width"),
            P("unit", "zero", "width"),
            P("unit", "zero", "width"),
        ),
        out_specs=(P("unit", "zero", "width"), P("unit", "zero", "width")),
        check_vma=False,
    )
```

```python
import functools

import jax
import jax.numpy as jnp
from jax import lax
from jax.experimental import pallas as pl
from jax.experimental.pallas import tpu as pltpu
from jax.sharding import PartitionSpec as P

ITERS = 3
GATHER_FROM = 1
RESULT_FROM = 1
CHUNKS = (4, 2, 1)
PARTS = (8, 4, 2, 1)
AHEAD = 2
MESH = pl.DeviceIdType.MESH


hold_rate = 0.95
learn_rate = 0.8
decay_rate = 0.1
keep_rate = 1.0 - learn_rate * decay_rate


def split(value):
    high = value.astype(jnp.bfloat16)
    low = (value - high.astype(jnp.float32)).astype(jnp.bfloat16)
    return high, low


def product(left, right, over):
    dims = (((1,), (over,)), ((), ()))
    dot = functools.partial(lax.dot_general, dimension_numbers=dims, preferred_element_type=jnp.float32)
    (lh, ll), (rh, rl) = left, right
    return dot(lh, rh) + (dot(lh, rl) + dot(ll, rh))


def orders(count):
    near = list(range(1, count))
    return near[GATHER_FROM:] + near[:GATHER_FROM], near[RESULT_FROM:] + near[:RESULT_FROM]


def paired(index, d, count):
    if d == 0:
        return index
    out, bit = 0, 1
    while bit < count:
        out = out + bit * ((index // bit + d // bit) % 2)
        bit *= 2
    return out


def factor(gram):
    side = gram.shape[0]
    rows = lax.broadcasted_iota(jnp.int32, (side, side), 0)
    cols = lax.broadcasted_iota(jnp.int32, (side, side), 1)
    eye = jnp.where(rows == cols, 1.0, 0.0).astype(jnp.float32)
    total = jnp.sum(jnp.sum(gram * eye, axis=1, keepdims=True), axis=0, keepdims=True)
    scale = lax.rsqrt(total + 1e-06)
    gram = gram * (scale * scale)
    held = None
    for step in range(ITERS):
        gs = split(gram)
        mixed = 3.4445 * eye - 4.775 * gram + 2.0315 * product(gs, gs, 0)
        ms = split(mixed)
        held = mixed if held is None else product(ms, split(held), 0)
        if step < ITERS - 1:
            gram = product(split(product(ms, gs, 0)), ms, 0)
    return held * scale


def kernel(nz, nw, chunks, per, grad, moment, weight, new_weights, new_momentum,
           grads, moments, weights, gather, grams, result, back,
           l_sem, w_sem, g_send, g_recv, p_send, p_recv, r_send, r_recv, column, all_in):
    zi, wi = lax.axis_index("zero"), lax.axis_index("width")
    mats = chunks * per
    rows, cols = grad.shape[1], grad.shape[2]
    side = nz * rows
    gather_order, result_order = orders(nz)
    ahead = min(AHEAD, chunks)
    far = nz - 1
    pieces = [(far, k) for k in range(ahead)]
    pieces += [(d, k) for k in range(ahead) for d in gather_order if d != far]
    pieces += [(d, k) for k in range(ahead, chunks) for d in gather_order]
    pieces += [(0, k) for k in range(chunks)]
    inners = (nz // 2 - 1, nz // 2)
    outers = [z for z in range(nz) if z not in inners]
    inner = (zi == inners[0]) | (zi == inners[1])
    outer = jnp.logical_not(inner)

    def partner(d):
        return paired(zi, d, nz)

    barrier = pltpu.get_barrier_semaphore()

    def tell(sem, axis, index):
        pl.semaphore_signal(sem, inc=1, device_id={axis: index}, device_id_type=MESH)

    @pl.when(inner)
    def _():
        tell(barrier, "zero", partner(far))

    for z in outers:
        @pl.when(zi != z)
        def _():
            tell(barrier, "zero", z)

    @pl.when(outer)
    def _():
        for d in range(1, nw):
            tell(barrier, "width", lax.rem(wi + d, nw))

    def piece(d, k):
        return pl.ds(partner(d) * mats + k * per, per)

    def group(n):
        return 0 if n == 0 else 1 + n // nz

    def load(which, n):
        source, target = ((grad, grads), (moment, moments))[which]
        return pltpu.make_async_copy(source.at[piece(*pieces[n])], target.at[piece(*pieces[n])], l_sem.at[group(n)])

    def load_weight():
        return pltpu.make_async_copy(weight, weights, w_sem.at[0])

    def wait_all(sem, *refs):
        for ref in refs:
            pltpu.make_async_copy(ref, ref, sem).wait()

    def gather_copy(d, k):
        return pltpu.make_async_remote_copy(
            src_ref=new_momentum.at[piece(d, k)],
            dst_ref=gather.at[zi, pl.ds(k * per, per)],
            send_sem=g_send.at[0], recv_sem=g_recv.at[k],
            device_id={"zero": partner(d)}, device_id_type=MESH)

    def gram_copy(d, k):
        return pltpu.make_async_remote_copy(
            src_ref=grams.at[wi, pl.ds(k * per, per)],
            dst_ref=grams.at[wi, pl.ds(k * per, per)],
            send_sem=p_send.at[0], recv_sem=p_recv.at[k],
            device_id={"width": lax.rem(wi + d, nw)}, device_id_type=MESH)

    def result_copy(d, k):
        return pltpu.make_async_remote_copy(
            src_ref=result.at[partner(d), pl.ds(k * per, per)],
            dst_ref=back.at[piece(0, k)],
            send_sem=r_send.at[0], recv_sem=r_recv.at[k],
            device_id={"zero": partner(d)}, device_id_type=MESH)

    for n in range(len(pieces)):
        load(0, n).start()
        load(1, n).start()

    def momentum(n):
        d, k = pieces[n]
        if n == 0 or group(n) != group(n - 1):
            members = sum(group(m) == group(n) for m in range(len(pieces)))
            wait_all(l_sem.at[group(n)], grads.at[pl.ds(0, 2 * members * per)])
        value = hold_rate * moments[piece(d, k)] + grads[piece(d, k)]
        new_momentum[piece(d, k)] = value
        if d == 0:
            gather[zi, pl.ds(k * per, per)] = value

    def release(d, k):
        if d:
            gather_copy(d, k).start()

    for n in range(len(pieces)):
        momentum(n)
        if n == 1:
            pl.semaphore_wait(barrier, jnp.where(inner, 1, nz + nw - 2))

            @pl.when(outer)
            def _():
                for z in inners:
                    tell(column, "zero", z)
                for d in range(1, nw):
                    tell(all_in, "width", lax.rem(wi + d, nw))
        if n == ahead + 1:
            @pl.when(inner)
            def _():
                pl.semaphore_wait(column, len(outers))
        if n:
            release(*pieces[n - 1])
    release(*pieces[-1])
    load_weight().start()

    @pl.when(outer)
    def _():
        pl.semaphore_wait(all_in, nw - 1)
        for z in inners:
            tell(all_in, "zero", z)

    def whole(i):
        return split(gather[:, i].reshape(side, cols))

    def finish(k):
        wait_all(p_recv.at[k], grams.at[pl.ds(0, nw - 1), pl.ds(k * per, per)])

        def one(j, carry):
            i = k * per + j
            gram = grams[0, i]
            for w in range(1, nw):
                gram = gram + grams[w, i]
            out = product(split(factor(gram)), whole(i), 0)
            result[:, i] = out.reshape(nz, rows, cols)
            return carry

        lax.fori_loop(0, per, one, 0)
        for d in result_order:
            result_copy(d, k).start()

    for k in range(chunks):
        wait_all(g_recv.at[k], gather.at[pl.ds(0, nz - 1), pl.ds(k * per, per)])

        def make(j, carry):
            i = k * per + j
            x = whole(i)
            grams[wi, i] = product(x, x, 1)
            return carry

        lax.fori_loop(0, per, make, 0)
        if k == 0:
            @pl.when(inner)
            def _():
                pl.semaphore_wait(all_in, len(outers))
        for d in range(1, nw):
            gram_copy(d, k).start()
        finish(k)

    load_weight().wait()
    for k in range(chunks):
        new_weights[piece(0, k)] = keep_rate * weights[piece(0, k)] - learn_rate * result[zi, pl.ds(k * per, per)]
    for k in range(chunks):
        wait_all(r_recv.at[k], back.at[pl.ds(0, (nz - 1) * per)])
        for d in result_order:
            new_weights[piece(d, k)] = keep_rate * weights[piece(d, k)] - learn_rate * back[piece(d, k)]

    wait_all(g_send.at[0], gather.at[pl.ds(0, nz - 1)])
    wait_all(p_send.at[0], grams.at[pl.ds(0, nw - 1)])
    wait_all(r_send.at[0], result.at[pl.ds(0, nz - 1)])


def store(*refs):
    count = len(refs) // 2
    sem = refs[-1]
    length = refs[0].shape[0]
    parts = next(p for p in PARTS if length % p == 0)
    for p in range(parts):
        part = pl.ds(p * length // parts, length // parts)
        for n in range(count):
            pltpu.make_async_copy(refs[n].at[part], refs[count + n].at[part], sem.at[n]).start()
    for n in range(count):
        pltpu.make_async_copy(refs[n], refs[count + n], sem.at[n]).wait()


def stored(*arrays):
    inside = pl.BlockSpec(memory_space=pltpu.VMEM)
    return pl.pallas_call(
        store,
        out_shape=tuple(pltpu.HBM(x.shape, x.dtype) for x in arrays),
        in_specs=[inside] * len(arrays),
        out_specs=(pl.BlockSpec(memory_space=pltpu.HBM),) * len(arrays),
        scratch_shapes=[pltpu.SemaphoreType.DMA((len(arrays),))],
        compiler_params=pltpu.CompilerParams(vmem_limit_bytes=2**20),
    )(*(pltpu.with_memory_space_constraint(x, pltpu.VMEM) for x in arrays))


def by_kernel(nz, nw, grad, moment, weight):
    total, rows, cols = grad.shape
    side, mats = nz * rows, total // nz
    chunks = next(c for c in CHUNKS if mats % c == 0)
    dma = pltpu.SemaphoreType.DMA
    anywhere = pl.BlockSpec(memory_space=pl.ANY)
    shape = pltpu.VMEM(grad.shape, jnp.float32)
    local = pltpu.VMEM((total, rows, cols), jnp.float32)
    shared = pltpu.VMEM((nz, mats, rows, cols), jnp.float32)
    results = pl.pallas_call(
        functools.partial(kernel, nz, nw, chunks, mats // chunks),
        out_shape=(shape, shape),
        in_specs=[anywhere] * 3,
        out_specs=(pl.BlockSpec(memory_space=pltpu.VMEM),) * 2,
        scratch_shapes=[
            local, local, local,
            shared,
            pltpu.VMEM((nw, mats, side, side), jnp.float32),
            shared,
            local,
            dma((chunks + 1,)), dma((1,)),
            dma((1,)), dma((chunks,)),
            dma((1,)), dma((chunks,)),
            dma((1,)), dma((chunks,)),
            pltpu.SemaphoreType.REGULAR, pltpu.SemaphoreType.REGULAR,
        ],
        compiler_params=pltpu.CompilerParams(
            collective_id=0, has_side_effects=True, vmem_limit_bytes=40 * 2**20),
    )(*(pltpu.with_memory_space_constraint(x, pltpu.HBM) for x in (grad, moment, weight)))
    return stored(*results)


def by_ops(new_momentum):
    moved = lax.all_to_all(new_momentum, "zero", split_axis=0, concat_axis=1, tiled=True)
    gram = jnp.einsum("mik,mjk->mij", moved, moved, precision=lax.Precision.HIGHEST)
    gram = lax.psum(gram, "width")
    eye = jnp.eye(gram.shape[1], dtype=jnp.float32)
    scale = lax.rsqrt(jnp.sum(gram * eye, axis=(1, 2), keepdims=True) + 1e-06)
    gram = gram * (scale * scale)
    dot = functools.partial(jnp.einsum, "mij,mjk->mik", precision=lax.Precision.HIGHEST)
    held = None
    for step in range(ITERS):
        mixed = 3.4445 * eye - 4.775 * gram + 2.0315 * dot(gram, gram)
        held = mixed if held is None else dot(mixed, held)
        gram = dot(dot(mixed, gram), mixed)
    out = dot(held * scale, moved)
    return lax.all_to_all(out, "zero", split_axis=1, concat_axis=0, tiled=True)


def body(nz, nw, grad_stack, moment_stack, weight_stack):
    if grad_stack.shape[1] % 8 == 0 and nz & (nz - 1) == 0 and nz > 2:
        return by_kernel(nz, nw, grad_stack, moment_stack, weight_stack)
    new_momentum = hold_rate * moment_stack + grad_stack
    new_weights = keep_rate * weight_stack - learn_rate * by_ops(new_momentum)
    return (new_weights, new_momentum)


def solution(mesh):
    return jax.shard_map(
        functools.partial(body, mesh.shape["zero"], mesh.shape["width"]),
        mesh=mesh,
        in_specs=(
            P("unit", "zero", "width"),
            P("unit", "zero", "width"),
            P("unit", "zero", "width"),
        ),
        out_specs=(P("unit", "zero", "width"), P("unit", "zero", "width")),
        check_vma=False,
    )
```

```python
import functools

import jax
import jax.numpy as jnp
from jax import lax
from jax.experimental import pallas as pl
from jax.experimental.pallas import tpu as pltpu
from jax.sharding import PartitionSpec as P

ITERS = 3
GATHER_FROM = 1
RESULT_FROM = 1
CHUNKS = (4, 2, 1)
PARTS = (8, 4, 2, 1)
AHEAD = 2
MESH = pl.DeviceIdType.MESH


hold_rate = 0.95
learn_rate = 0.8
decay_rate = 0.1
keep_rate = 1.0 - learn_rate * decay_rate


def split(value):
    high = value.astype(jnp.bfloat16)
    low = (value - high.astype(jnp.float32)).astype(jnp.bfloat16)
    return high, low


def product(left, right, over):
    dims = (((1,), (over,)), ((), ()))
    dot = functools.partial(lax.dot_general, dimension_numbers=dims, preferred_element_type=jnp.float32)
    (lh, ll), (rh, rl) = left, right
    return dot(lh, rh) + (dot(lh, rl) + dot(ll, rh))


def orders(count):
    near = list(range(1, count))
    return near[GATHER_FROM:] + near[:GATHER_FROM], near[RESULT_FROM:] + near[:RESULT_FROM]


def paired(index, d, count):
    if d == 0:
        return index
    out, bit = 0, 1
    while bit < count:
        out = out + bit * ((index // bit + d // bit) % 2)
        bit *= 2
    return out


def factor(gram):
    side = gram.shape[0]
    rows = lax.broadcasted_iota(jnp.int32, (side, side), 0)
    cols = lax.broadcasted_iota(jnp.int32, (side, side), 1)
    eye = jnp.where(rows == cols, 1.0, 0.0).astype(jnp.float32)
    total = jnp.sum(jnp.sum(gram * eye, axis=1, keepdims=True), axis=0, keepdims=True)
    scale = lax.rsqrt(total + 1e-06)
    gram = gram * (scale * scale)
    held = None
    for step in range(ITERS):
        gs = split(gram)
        mixed = 3.4445 * eye - 4.775 * gram + 2.0315 * product(gs, gs, 0)
        ms = split(mixed)
        held = mixed if held is None else product(ms, split(held), 0)
        if step < ITERS - 1:
            gram = product(split(product(ms, gs, 0)), ms, 0)
    return held * scale


def kernel(nz, nw, chunks, per, grad, moment, weight, new_weights, new_momentum,
           grads, moments, weights, gather, grams, result, back,
           l_sem, w_sem, g_send, g_recv, p_send, p_recv, r_send, r_recv, column, all_in):
    zi, wi = lax.axis_index("zero"), lax.axis_index("width")
    mats = chunks * per
    rows, cols = grad.shape[1], grad.shape[2]
    side = nz * rows
    gather_order, result_order = orders(nz)
    ahead = min(AHEAD, chunks)
    far = nz - 1
    pieces = [(far, k) for k in range(ahead)]
    pieces += [(d, k) for k in range(ahead) for d in gather_order if d != far]
    pieces += [(d, k) for k in range(ahead, chunks) for d in gather_order]
    pieces += [(0, k) for k in range(chunks)]
    inners = (nz // 2 - 1, nz // 2)
    outers = [z for z in range(nz) if z not in inners]
    inner = (zi == inners[0]) | (zi == inners[1])
    outer = jnp.logical_not(inner)

    def partner(d):
        return paired(zi, d, nz)

    barrier = pltpu.get_barrier_semaphore()

    def tell(sem, axis, index):
        pl.semaphore_signal(sem, inc=1, device_id={axis: index}, device_id_type=MESH)

    def piece(d, k):
        return pl.ds(partner(d) * mats + k * per, per)

    def group(n):
        return 0 if n == 0 else 1 + n // nz

    def load(which, n):
        source, target = ((grad, grads), (moment, moments))[which]
        return pltpu.make_async_copy(source.at[piece(*pieces[n])], target.at[piece(*pieces[n])], l_sem.at[group(n)])

    def load_weight():
        return pltpu.make_async_copy(weight, weights, w_sem.at[0])

    def wait_all(sem, *refs):
        for ref in refs:
            pltpu.make_async_copy(ref, ref, sem).wait()

    def gather_copy(d, k):
        return pltpu.make_async_remote_copy(
            src_ref=new_momentum.at[piece(d, k)],
            dst_ref=gather.at[zi, pl.ds(k * per, per)],
            send_sem=g_send.at[0], recv_sem=g_recv.at[k],
            device_id={"zero": partner(d)}, device_id_type=MESH)

    def gram_copy(d, k):
        return pltpu.make_async_remote_copy(
            src_ref=grams.at[wi, pl.ds(k * per, per)],
            dst_ref=grams.at[wi, pl.ds(k * per, per)],
            send_sem=p_send.at[0], recv_sem=p_recv.at[k],
            device_id={"width": lax.rem(wi + d, nw)}, device_id_type=MESH)

    def result_copy(d, k):
        return pltpu.make_async_remote_copy(
            src_ref=result.at[partner(d), pl.ds(k * per, per)],
            dst_ref=back.at[piece(0, k)],
            send_sem=r_send.at[0], recv_sem=r_recv.at[k],
            device_id={"zero": partner(d)}, device_id_type=MESH)

    @pl.when(inner)
    def _():
        tell(barrier, "zero", partner(far))

    load(0, 0).start()
    load(1, 0).start()
    for z in outers:
        @pl.when(zi != z)
        def _():
            tell(barrier, "zero", z)

    @pl.when(outer)
    def _():
        for d in range(1, nw):
            tell(barrier, "width", lax.rem(wi + d, nw))

    for n in range(1, len(pieces)):
        load(0, n).start()
        load(1, n).start()

    def momentum(n):
        d, k = pieces[n]
        if n == 0 or group(n) != group(n - 1):
            members = sum(group(m) == group(n) for m in range(len(pieces)))
            wait_all(l_sem.at[group(n)], grads.at[pl.ds(0, 2 * members * per)])
        value = hold_rate * moments[piece(d, k)] + grads[piece(d, k)]
        new_momentum[piece(d, k)] = value
        if d == 0:
            gather[zi, pl.ds(k * per, per)] = value

    def release(d, k):
        if d:
            gather_copy(d, k).start()

    for n in range(len(pieces)):
        momentum(n)
        if n == 0:
            pl.semaphore_wait(barrier, jnp.where(inner, 1, nz + nw - 2))
            release(*pieces[0])

            @pl.when(outer)
            def _():
                for z in inners:
                    tell(column, "zero", z)
                for d in range(1, nw):
                    tell(all_in, "width", lax.rem(wi + d, nw))
        if n == ahead + 1:
            @pl.when(inner)
            def _():
                pl.semaphore_wait(column, len(outers))
        if n > 1:
            release(*pieces[n - 1])
    release(*pieces[-1])
    load_weight().start()

    @pl.when(outer)
    def _():
        pl.semaphore_wait(all_in, nw - 1)
        for z in inners:
            tell(all_in, "zero", z)

    def whole(i):
        return split(gather[:, i].reshape(side, cols))

    def finish(k):
        wait_all(p_recv.at[k], grams.at[pl.ds(0, nw - 1), pl.ds(k * per, per)])

        def one(j, carry):
            i = k * per + j
            gram = grams[0, i]
            for w in range(1, nw):
                gram = gram + grams[w, i]
            out = product(split(factor(gram)), whole(i), 0)
            result[:, i] = out.reshape(nz, rows, cols)
            return carry

        lax.fori_loop(0, per, one, 0)
        results = [(d, k) for d in result_order if d != far]
        if k > 0:
            results.insert(1, (far, k - 1))
        if k == chunks - 1:
            results.append((far, k))
        for piece_of in results:
            result_copy(*piece_of).start()

    for k in range(chunks):
        wait_all(g_recv.at[k], gather.at[pl.ds(0, nz - 1), pl.ds(k * per, per)])

        def make(j, carry):
            i = k * per + j
            x = whole(i)
            grams[wi, i] = product(x, x, 1)
            return carry

        lax.fori_loop(0, per, make, 0)
        if k == 0:
            @pl.when(inner)
            def _():
                pl.semaphore_wait(all_in, len(outers))
        for d in range(1, nw):
            gram_copy(d, k).start()
        finish(k)

    load_weight().wait()
    for k in range(chunks):
        new_weights[piece(0, k)] = keep_rate * weights[piece(0, k)] - learn_rate * result[zi, pl.ds(k * per, per)]
    for k in range(chunks):
        wait_all(r_recv.at[k], back.at[pl.ds(0, (nz - 1) * per)])
        for d in result_order:
            new_weights[piece(d, k)] = keep_rate * weights[piece(d, k)] - learn_rate * back[piece(d, k)]

    wait_all(g_send.at[0], gather.at[pl.ds(0, nz - 1)])
    wait_all(p_send.at[0], grams.at[pl.ds(0, nw - 1)])
    wait_all(r_send.at[0], result.at[pl.ds(0, nz - 1)])


def store(*refs):
    count = len(refs) // 2
    sem = refs[-1]
    length = refs[0].shape[0]
    parts = next(p for p in PARTS if length % p == 0)
    for p in range(parts):
        part = pl.ds(p * length // parts, length // parts)
        for n in range(count):
            pltpu.make_async_copy(refs[n].at[part], refs[count + n].at[part], sem.at[n]).start()
    for n in range(count):
        pltpu.make_async_copy(refs[n], refs[count + n], sem.at[n]).wait()


def stored(*arrays):
    inside = pl.BlockSpec(memory_space=pltpu.VMEM)
    return pl.pallas_call(
        store,
        out_shape=tuple(pltpu.HBM(x.shape, x.dtype) for x in arrays),
        in_specs=[inside] * len(arrays),
        out_specs=(pl.BlockSpec(memory_space=pltpu.HBM),) * len(arrays),
        scratch_shapes=[pltpu.SemaphoreType.DMA((len(arrays),))],
        compiler_params=pltpu.CompilerParams(vmem_limit_bytes=2**20),
    )(*(pltpu.with_memory_space_constraint(x, pltpu.VMEM) for x in arrays))


def by_kernel(nz, nw, grad, moment, weight):
    total, rows, cols = grad.shape
    side, mats = nz * rows, total // nz
    chunks = next(c for c in CHUNKS if mats % c == 0)
    dma = pltpu.SemaphoreType.DMA
    anywhere = pl.BlockSpec(memory_space=pl.ANY)
    shape = pltpu.VMEM(grad.shape, jnp.float32)
    local = pltpu.VMEM((total, rows, cols), jnp.float32)
    shared = pltpu.VMEM((nz, mats, rows, cols), jnp.float32)
    results = pl.pallas_call(
        functools.partial(kernel, nz, nw, chunks, mats // chunks),
        out_shape=(shape, shape),
        in_specs=[anywhere] * 3,
        out_specs=(pl.BlockSpec(memory_space=pltpu.VMEM),) * 2,
        scratch_shapes=[
            local, local, local,
            shared,
            pltpu.VMEM((nw, mats, side, side), jnp.float32),
            shared,
            local,
            dma((chunks + 1,)), dma((1,)),
            dma((1,)), dma((chunks,)),
            dma((1,)), dma((chunks,)),
            dma((1,)), dma((chunks,)),
            pltpu.SemaphoreType.REGULAR, pltpu.SemaphoreType.REGULAR,
        ],
        compiler_params=pltpu.CompilerParams(
            collective_id=0, has_side_effects=True, vmem_limit_bytes=40 * 2**20),
    )(*(pltpu.with_memory_space_constraint(x, pltpu.HBM) for x in (grad, moment, weight)))
    return stored(*results)


def by_ops(new_momentum):
    moved = lax.all_to_all(new_momentum, "zero", split_axis=0, concat_axis=1, tiled=True)
    gram = jnp.einsum("mik,mjk->mij", moved, moved, precision=lax.Precision.HIGHEST)
    gram = lax.psum(gram, "width")
    eye = jnp.eye(gram.shape[1], dtype=jnp.float32)
    scale = lax.rsqrt(jnp.sum(gram * eye, axis=(1, 2), keepdims=True) + 1e-06)
    gram = gram * (scale * scale)
    dot = functools.partial(jnp.einsum, "mij,mjk->mik", precision=lax.Precision.HIGHEST)
    held = None
    for step in range(ITERS):
        mixed = 3.4445 * eye - 4.775 * gram + 2.0315 * dot(gram, gram)
        held = mixed if held is None else dot(mixed, held)
        gram = dot(dot(mixed, gram), mixed)
    out = dot(held * scale, moved)
    return lax.all_to_all(out, "zero", split_axis=1, concat_axis=0, tiled=True)


def body(nz, nw, grad_stack, moment_stack, weight_stack):
    if grad_stack.shape[1] % 8 == 0 and nz & (nz - 1) == 0 and nz > 2:
        return by_kernel(nz, nw, grad_stack, moment_stack, weight_stack)
    new_momentum = hold_rate * moment_stack + grad_stack
    new_weights = keep_rate * weight_stack - learn_rate * by_ops(new_momentum)
    return (new_weights, new_momentum)


def solution(mesh):
    return jax.shard_map(
        functools.partial(body, mesh.shape["zero"], mesh.shape["width"]),
        mesh=mesh,
        in_specs=(
            P("unit", "zero", "width"),
            P("unit", "zero", "width"),
            P("unit", "zero", "width"),
        ),
        out_specs=(P("unit", "zero", "width"), P("unit", "zero", "width")),
        check_vma=False,
    )
```

```python
import functools

import jax
import jax.numpy as jnp
from jax import lax
from jax.experimental import pallas as pl
from jax.experimental.pallas import tpu as pltpu
from jax.sharding import PartitionSpec as P

ITERS = 3
GATHER_FROM = 1
RESULT_FROM = 1
CHUNKS = (4, 2, 1)
PARTS = (16, 8, 4, 2, 1)
AHEAD = 2
MESH = pl.DeviceIdType.MESH


hold_rate = 0.95
learn_rate = 0.8
decay_rate = 0.1
keep_rate = 1.0 - learn_rate * decay_rate


def split(value):
    high = value.astype(jnp.bfloat16)
    low = (value - high.astype(jnp.float32)).astype(jnp.bfloat16)
    return high, low


def product(left, right, over):
    dims = (((1,), (over,)), ((), ()))
    dot = functools.partial(lax.dot_general, dimension_numbers=dims, preferred_element_type=jnp.float32)
    (lh, ll), (rh, rl) = left, right
    return dot(lh, rh) + (dot(lh, rl) + dot(ll, rh))


def orders(count):
    near = list(range(1, count))
    return near[GATHER_FROM:] + near[:GATHER_FROM], near[RESULT_FROM:] + near[:RESULT_FROM]


def paired(index, d, count):
    if d == 0:
        return index
    out, bit = 0, 1
    while bit < count:
        out = out + bit * ((index // bit + d // bit) % 2)
        bit *= 2
    return out


def factor(gram):
    side = gram.shape[0]
    rows = lax.broadcasted_iota(jnp.int32, (side, side), 0)
    cols = lax.broadcasted_iota(jnp.int32, (side, side), 1)
    eye = jnp.where(rows == cols, 1.0, 0.0).astype(jnp.float32)
    total = jnp.sum(jnp.sum(gram * eye, axis=1, keepdims=True), axis=0, keepdims=True)
    scale = lax.rsqrt(total + 1e-06)
    gram = gram * (scale * scale)
    held = None
    for step in range(ITERS):
        gs = split(gram)
        mixed = 3.4445 * eye - 4.775 * gram + 2.0315 * product(gs, gs, 0)
        ms = split(mixed)
        held = mixed if held is None else product(ms, split(held), 0)
        if step < ITERS - 1:
            gram = product(split(product(ms, gs, 0)), ms, 0)
    return held * scale


def kernel(nz, nw, chunks, per, grad, moment, weight, new_weights, new_momentum,
           grads, moments, weights, gather, grams, result, back,
           l_sem, w_sem, g_send, g_recv, p_send, p_recv, r_send, r_recv, column, all_in):
    zi, wi = lax.axis_index("zero"), lax.axis_index("width")
    mats = chunks * per
    rows, cols = grad.shape[1], grad.shape[2]
    side = nz * rows
    gather_order, result_order = orders(nz)
    ahead = min(AHEAD, chunks)
    far = nz - 1
    pieces = [(far, k) for k in range(ahead)]
    pieces += [(d, k) for k in range(ahead) for d in gather_order if d != far]
    pieces += [(d, k) for k in range(ahead, chunks) for d in gather_order]
    pieces += [(0, k) for k in range(chunks)]
    inners = (nz // 2 - 1, nz // 2)
    outers = [z for z in range(nz) if z not in inners]
    inner = (zi == inners[0]) | (zi == inners[1])
    outer = jnp.logical_not(inner)

    def partner(d):
        return paired(zi, d, nz)

    barrier = pltpu.get_barrier_semaphore()

    def tell(sem, axis, index):
        pl.semaphore_signal(sem, inc=1, device_id={axis: index}, device_id_type=MESH)

    def piece(d, k):
        return pl.ds(partner(d) * mats + k * per, per)

    def group(n):
        return 0 if n == 0 else 1 + 2 * n // len(pieces)

    def load(which, n):
        source, target = ((grad, grads), (moment, moments))[which]
        return pltpu.make_async_copy(source.at[piece(*pieces[n])], target.at[piece(*pieces[n])], l_sem.at[group(n)])

    def load_weight():
        return pltpu.make_async_copy(weight, weights, w_sem.at[0])

    def wait_all(sem, *refs):
        for ref in refs:
            pltpu.make_async_copy(ref, ref, sem).wait()

    def gather_copy(d, k):
        return pltpu.make_async_remote_copy(
            src_ref=new_momentum.at[piece(d, k)],
            dst_ref=gather.at[zi, pl.ds(k * per, per)],
            send_sem=g_send.at[0], recv_sem=g_recv.at[k],
            device_id={"zero": partner(d)}, device_id_type=MESH)

    def gram_copy(d, k):
        return pltpu.make_async_remote_copy(
            src_ref=grams.at[wi, pl.ds(k * per, per)],
            dst_ref=grams.at[wi, pl.ds(k * per, per)],
            send_sem=p_send.at[0], recv_sem=p_recv.at[k],
            device_id={"width": lax.rem(wi + d, nw)}, device_id_type=MESH)

    def result_copy(d, k):
        return pltpu.make_async_remote_copy(
            src_ref=result.at[partner(d), pl.ds(k * per, per)],
            dst_ref=back.at[piece(0, k)],
            send_sem=r_send.at[0], recv_sem=r_recv.at[int(k == chunks - 1)],
            device_id={"zero": partner(d)}, device_id_type=MESH)

    @pl.when(inner)
    def _():
        tell(barrier, "zero", partner(far))

    for i in range(per):
        for row in range(0, rows, 8):
            for source, target in ((grad, grads), (moment, moments)):
                part = (partner(far) * mats + i, pl.ds(row, 8))
                pltpu.make_async_copy(source.at[part], target.at[part], l_sem.at[0]).start()
    for z in outers:
        @pl.when(zi != z)
        def _():
            tell(barrier, "zero", z)

    @pl.when(outer)
    def _():
        for d in range(1, nw):
            tell(barrier, "width", lax.rem(wi + d, nw))

    for n in range(1, len(pieces)):
        load(0, n).start()
        load(1, n).start()

    def momentum(n):
        d, k = pieces[n]
        if n == 0 or group(n) != group(n - 1):
            members = sum(group(m) == group(n) for m in range(len(pieces)))
            wait_all(l_sem.at[group(n)], grads.at[pl.ds(0, 2 * members * per)])
        value = hold_rate * moments[piece(d, k)] + grads[piece(d, k)]
        new_momentum[piece(d, k)] = value
        if d == 0:
            gather[zi, pl.ds(k * per, per)] = value

    def release(d, k):
        if d:
            gather_copy(d, k).start()

    for n in range(len(pieces)):
        momentum(n)
        if n == 0:
            pl.semaphore_wait(barrier, jnp.where(inner, 1, nz + nw - 2))
            release(*pieces[0])

            @pl.when(outer)
            def _():
                for z in inners:
                    tell(column, "zero", z)
                for d in range(1, nw):
                    tell(all_in, "width", lax.rem(wi + d, nw))
        if n == ahead + 1:
            @pl.when(inner)
            def _():
                pl.semaphore_wait(column, len(outers))
        if n > 1:
            release(*pieces[n - 1])
    release(*pieces[-1])
    load_weight().start()

    @pl.when(outer)
    def _():
        pl.semaphore_wait(all_in, nw - 1)
        for z in inners:
            tell(all_in, "zero", z)

    def whole(i):
        return split(gather[:, i].reshape(side, cols))

    def finish(k):
        wait_all(p_recv.at[k], grams.at[pl.ds(0, nw - 1), pl.ds(k * per, per)])

        def one(j, carry):
            i = k * per + j
            gram = grams[0, i]
            for w in range(1, nw):
                gram = gram + grams[w, i]
            out = product(split(factor(gram)), whole(i), 0)
            result[:, i] = out.reshape(nz, rows, cols)
            return carry

        lax.fori_loop(0, per, one, 0)
        results = [(d, k) for d in result_order if d != far]
        if k > 0:
            results.insert(1, (far, k - 1))
        if k == chunks - 1:
            results.append((far, k))
        for piece_of in results:
            result_copy(*piece_of).start()

    def begin(k):
        wait_all(g_recv.at[k], gather.at[pl.ds(0, nz - 1), pl.ds(k * per, per)])

        def make(j, carry):
            i = k * per + j
            x = whole(i)
            grams[wi, i] = product(x, x, 1)
            return carry

        lax.fori_loop(0, per, make, 0)
        if k == 0:
            @pl.when(inner)
            def _():
                pl.semaphore_wait(all_in, len(outers))
        for d in range(1, nw):
            gram_copy(d, k).start()

    for k in range(ahead):
        begin(k)
    for k in range(ahead):
        finish(k)
    for k in range(ahead, chunks):
        begin(k)
        finish(k)

    load_weight().wait()
    for k in range(chunks):
        new_weights[piece(0, k)] = keep_rate * weights[piece(0, k)] - learn_rate * result[zi, pl.ds(k * per, per)]
    wait_all(g_send.at[0], gather.at[pl.ds(0, nz - 1)])
    wait_all(p_send.at[0], grams.at[pl.ds(0, nw - 1)])
    for part, members in enumerate((range(chunks - 1), range(chunks - 1, chunks))):
        if members:
            wait_all(r_recv.at[part], back.at[pl.ds(0, (nz - 1) * per * len(members))])
        for k in members:
            for d in result_order:
                new_weights[piece(d, k)] = keep_rate * weights[piece(d, k)] - learn_rate * back[piece(d, k)]

    wait_all(r_send.at[0], result.at[pl.ds(0, nz - 1)])


def store(*refs):
    count = len(refs) // 2
    sem = refs[-1]
    length = refs[0].shape[0]
    parts = next(p for p in PARTS if length % p == 0)
    for p in range(parts):
        part = pl.ds(p * length // parts, length // parts)
        for n in range(count):
            pltpu.make_async_copy(refs[n].at[part], refs[count + n].at[part], sem.at[n]).start()
    for n in range(count):
        pltpu.make_async_copy(refs[n], refs[count + n], sem.at[n]).wait()


def stored(*arrays):
    inside = pl.BlockSpec(memory_space=pltpu.VMEM)
    return pl.pallas_call(
        store,
        out_shape=tuple(pltpu.HBM(x.shape, x.dtype) for x in arrays),
        in_specs=[inside] * len(arrays),
        out_specs=(pl.BlockSpec(memory_space=pltpu.HBM),) * len(arrays),
        scratch_shapes=[pltpu.SemaphoreType.DMA((len(arrays),))],
        compiler_params=pltpu.CompilerParams(vmem_limit_bytes=2**20),
    )(*(pltpu.with_memory_space_constraint(x, pltpu.VMEM) for x in arrays))


def by_kernel(nz, nw, grad, moment, weight):
    total, rows, cols = grad.shape
    side, mats = nz * rows, total // nz
    chunks = next(c for c in CHUNKS if mats % c == 0)
    dma = pltpu.SemaphoreType.DMA
    anywhere = pl.BlockSpec(memory_space=pl.ANY)
    shape = pltpu.VMEM(grad.shape, jnp.float32)
    local = pltpu.VMEM((total, rows, cols), jnp.float32)
    shared = pltpu.VMEM((nz, mats, rows, cols), jnp.float32)
    results = pl.pallas_call(
        functools.partial(kernel, nz, nw, chunks, mats // chunks),
        out_shape=(shape, shape),
        in_specs=[anywhere] * 3,
        out_specs=(pl.BlockSpec(memory_space=pltpu.VMEM),) * 2,
        scratch_shapes=[
            local, local, local,
            shared,
            pltpu.VMEM((nw, mats, side, side), jnp.float32),
            shared,
            local,
            dma((3,)), dma((1,)),
            dma((1,)), dma((chunks,)),
            dma((1,)), dma((chunks,)),
            dma((1,)), dma((2,)),
            pltpu.SemaphoreType.REGULAR, pltpu.SemaphoreType.REGULAR,
        ],
        compiler_params=pltpu.CompilerParams(
            collective_id=0, has_side_effects=True, vmem_limit_bytes=40 * 2**20),
    )(*(pltpu.with_memory_space_constraint(x, pltpu.HBM) for x in (grad, moment, weight)))
    return stored(*results)


def by_ops(new_momentum):
    moved = lax.all_to_all(new_momentum, "zero", split_axis=0, concat_axis=1, tiled=True)
    gram = jnp.einsum("mik,mjk->mij", moved, moved, precision=lax.Precision.HIGHEST)
    gram = lax.psum(gram, "width")
    eye = jnp.eye(gram.shape[1], dtype=jnp.float32)
    scale = lax.rsqrt(jnp.sum(gram * eye, axis=(1, 2), keepdims=True) + 1e-06)
    gram = gram * (scale * scale)
    dot = functools.partial(jnp.einsum, "mij,mjk->mik", precision=lax.Precision.HIGHEST)
    held = None
    for step in range(ITERS):
        mixed = 3.4445 * eye - 4.775 * gram + 2.0315 * dot(gram, gram)
        held = mixed if held is None else dot(mixed, held)
        gram = dot(dot(mixed, gram), mixed)
    out = dot(held * scale, moved)
    return lax.all_to_all(out, "zero", split_axis=1, concat_axis=0, tiled=True)


def body(nz, nw, grad_stack, moment_stack, weight_stack):
    if grad_stack.shape[1] % 8 == 0 and nz & (nz - 1) == 0 and nz > 2:
        return by_kernel(nz, nw, grad_stack, moment_stack, weight_stack)
    new_momentum = hold_rate * moment_stack + grad_stack
    new_weights = keep_rate * weight_stack - learn_rate * by_ops(new_momentum)
    return (new_weights, new_momentum)


def solution(mesh):
    return jax.shard_map(
        functools.partial(body, mesh.shape["zero"], mesh.shape["width"]),
        mesh=mesh,
        in_specs=(
            P("unit", "zero", "width"),
            P("unit", "zero", "width"),
            P("unit", "zero", "width"),
        ),
        out_specs=(P("unit", "zero", "width"), P("unit", "zero", "width")),
        check_vma=False,
    )
```

```python
import functools

import jax
import jax.numpy as jnp
from jax import lax
from jax.experimental import pallas as pl
from jax.experimental.pallas import tpu as pltpu
from jax.sharding import PartitionSpec as P

ITERS = 3
GATHER_FROM = 1
RESULT_FROM = 1
CHUNKS = (4, 2, 1)
PARTS = (32, 16, 8, 4, 2, 1)
AHEAD = 3
PLAN = 2
MESH = pl.DeviceIdType.MESH


hold_rate = 0.95
learn_rate = 0.8
decay_rate = 0.1
keep_rate = 1.0 - learn_rate * decay_rate


def split(value):
    high = value.astype(jnp.bfloat16)
    low = (value - high.astype(jnp.float32)).astype(jnp.bfloat16)
    return high, low


def product(left, right, over):
    dims = (((1,), (over,)), ((), ()))
    dot = functools.partial(lax.dot_general, dimension_numbers=dims, preferred_element_type=jnp.float32)
    (lh, ll), (rh, rl) = left, right
    return dot(lh, rh) + (dot(lh, rl) + dot(ll, rh))


def orders(count):
    near = list(range(1, count))
    return near[GATHER_FROM:] + near[:GATHER_FROM], near[RESULT_FROM:] + near[:RESULT_FROM]


def paired(index, d, count):
    if d == 0:
        return index
    out, bit = 0, 1
    while bit < count:
        out = out + bit * ((index // bit + d // bit) % 2)
        bit *= 2
    return out


def factor(gram):
    side = gram.shape[0]
    rows = lax.broadcasted_iota(jnp.int32, (side, side), 0)
    cols = lax.broadcasted_iota(jnp.int32, (side, side), 1)
    eye = jnp.where(rows == cols, 1.0, 0.0).astype(jnp.float32)
    total = jnp.sum(jnp.sum(gram * eye, axis=1, keepdims=True), axis=0, keepdims=True)
    scale = lax.rsqrt(total + 1e-06)
    gram = gram * (scale * scale)
    held = None
    for step in range(ITERS):
        gs = split(gram)
        mixed = 3.4445 * eye - 4.775 * gram + 2.0315 * product(gs, gs, 0)
        ms = split(mixed)
        held = mixed if held is None else product(ms, split(held), 0)
        if step < ITERS - 1:
            gram = product(split(product(ms, gs, 0)), ms, 0)
    return held * scale


def kernel(nz, nw, chunks, per, grad, moment, weight, new_weights, new_momentum,
           grads, moments, weights, gather, grams, result, back,
           l_sem, g_send, g_recv, p_recv, r_recv, column, all_in):
    zi, wi = lax.axis_index("zero"), lax.axis_index("width")
    mats = chunks * per
    rows, cols = grad.shape[1], grad.shape[2]
    side = nz * rows
    gather_order, result_order = orders(nz)
    ahead = min(AHEAD, chunks)
    far = nz - 1
    pieces = [(far, k) for k in range(ahead)]
    pieces += [(d, k) for k in range(ahead) for d in gather_order if d != far]
    pieces += [(d, k) for k in range(ahead, chunks) for d in gather_order]
    pieces += [(0, k) for k in range(chunks)]
    inners = (nz // 2 - 1, nz // 2)
    outers = [z for z in range(nz) if z not in inners]
    inner = (zi == inners[0]) | (zi == inners[1])
    outer = jnp.logical_not(inner)

    def partner(d):
        return paired(zi, d, nz)

    barrier = pltpu.get_barrier_semaphore()

    def tell(sem, axis, index):
        pl.semaphore_signal(sem, inc=1, device_id={axis: index}, device_id_type=MESH)

    def piece(d, k):
        return pl.ds(partner(d) * mats + k * per, per)

    def group(n):
        return 0 if n == 0 else 1 + 2 * n // len(pieces)

    def load(which, n):
        source, target = ((grad, grads), (moment, moments))[which]
        return pltpu.make_async_copy(source.at[piece(*pieces[n])], target.at[piece(*pieces[n])], l_sem.at[group(n)])

    def load_weight():
        return pltpu.make_async_copy(weight, weights, l_sem.at[0])

    def wait_all(sem, *refs):
        for ref in refs:
            pltpu.make_async_copy(ref, ref, sem).wait()

    def gather_copy(d, k):
        return pltpu.make_async_remote_copy(
            src_ref=new_momentum.at[piece(d, k)],
            dst_ref=gather.at[zi, pl.ds(k * per, per)],
            send_sem=g_send.at[0], recv_sem=g_recv.at[k],
            device_id={"zero": partner(d)}, device_id_type=MESH)

    def gram_copy(d, k):
        return pltpu.make_async_remote_copy(
            src_ref=grams.at[wi, pl.ds(k * per, per)],
            dst_ref=grams.at[wi, pl.ds(k * per, per)],
            send_sem=l_sem.at[1], recv_sem=p_recv.at[k],
            device_id={"width": lax.rem(wi + d, nw)}, device_id_type=MESH)

    def result_copy(d, k):
        return pltpu.make_async_remote_copy(
            src_ref=result.at[partner(d), pl.ds(k * per, per)],
            dst_ref=back.at[piece(0, k)],
            send_sem=l_sem.at[2], recv_sem=r_recv.at[int(k == chunks - 1)],
            device_id={"zero": partner(d)}, device_id_type=MESH)

    @pl.when(inner)
    def _():
        tell(barrier, "zero", partner(far))

    for i in range(per):
        for row in range(0, rows, 8):
            for source, target in ((grad, grads), (moment, moments)):
                part = (partner(far) * mats + i, pl.ds(row, 8))
                pltpu.make_async_copy(source.at[part], target.at[part], l_sem.at[0]).start()
    for z in outers:
        @pl.when(zi != z)
        def _():
            tell(barrier, "zero", z)

    @pl.when(outer)
    def _():
        for d in range(1, nw):
            tell(barrier, "width", lax.rem(wi + d, nw))

    for n in range(1, len(pieces)):
        load(0, n).start()
        load(1, n).start()

    def momentum(n):
        d, k = pieces[n]
        if n == 0 or group(n) != group(n - 1):
            members = sum(group(m) == group(n) for m in range(len(pieces)))
            wait_all(l_sem.at[group(n)], grads.at[pl.ds(0, 2 * members * per)])
        value = hold_rate * moments[piece(d, k)] + grads[piece(d, k)]
        new_momentum[piece(d, k)] = value
        if d == 0:
            gather[zi, pl.ds(k * per, per)] = value

    def release(d, k):
        if d:
            gather_copy(d, k).start()

    for n in range(len(pieces)):
        momentum(n)
        if n == 0:
            pl.semaphore_wait(barrier, jnp.where(inner, 1, nz + nw - 2))
            release(*pieces[0])

            @pl.when(outer)
            def _():
                for z in inners:
                    tell(column, "zero", z)
                for d in range(1, nw):
                    tell(all_in, "width", lax.rem(wi + d, nw))
        if n == ahead + 1:
            @pl.when(inner)
            def _():
                pl.semaphore_wait(column, len(outers))
        if n > 1:
            release(*pieces[n - 1])
    release(*pieces[-1])
    load_weight().start()

    @pl.when(outer)
    def _():
        pl.semaphore_wait(all_in, nw - 1)
        for z in inners:
            tell(all_in, "zero", z)

    def whole(i):
        return split(gather[:, i].reshape(side, cols))

    def finish(k):
        wait_all(p_recv.at[k], grams.at[pl.ds(0, nw - 1), pl.ds(k * per, per)])

        def one(j, carry):
            i = k * per + j
            gram = grams[0, i]
            for w in range(1, nw):
                gram = gram + grams[w, i]
            out = product(split(factor(gram)), whole(i), 0)
            result[:, i] = out.reshape(nz, rows, cols)
            return carry

        lax.fori_loop(0, per, one, 0)
        results = [(d, k) for d in result_order if d != far]
        if k > 0:
            results.insert(1, (far, k - 1))
        if k == chunks - 1:
            results.append((far, k))
        for piece_of in results:
            result_copy(*piece_of).start()

    def begin(k):
        wait_all(g_recv.at[k], gather.at[pl.ds(0, nz - 1), pl.ds(k * per, per)])

        def make(j, carry):
            i = k * per + j
            x = whole(i)
            grams[wi, i] = product(x, x, 1)
            return carry

        lax.fori_loop(0, per, make, 0)
        if k == 0:
            @pl.when(inner)
            def _():
                pl.semaphore_wait(all_in, len(outers))
        for d in range(1, nw):
            gram_copy(d, k).start()

    for k in range(min(PLAN, chunks)):
        begin(k)
    for k in range(min(PLAN, chunks)):
        finish(k)
    for k in range(min(PLAN, chunks), chunks):
        begin(k)
        finish(k)

    load_weight().wait()
    for k in range(chunks):
        new_weights[piece(0, k)] = keep_rate * weights[piece(0, k)] - learn_rate * result[zi, pl.ds(k * per, per)]
    wait_all(g_send.at[0], gather.at[pl.ds(0, nz - 1)])
    wait_all(l_sem.at[1], grams.at[pl.ds(0, nw - 1)])
    for part, members in enumerate((range(chunks - 1), range(chunks - 1, chunks))):
        if members:
            wait_all(r_recv.at[part], back.at[pl.ds(0, (nz - 1) * per * len(members))])
        for k in members:
            for d in result_order:
                new_weights[piece(d, k)] = keep_rate * weights[piece(d, k)] - learn_rate * back[piece(d, k)]

    wait_all(l_sem.at[2], result.at[pl.ds(0, nz - 1)])


def store(*refs):
    count = len(refs) // 2
    sem = refs[-1]
    length = refs[0].shape[0]
    parts = next(p for p in PARTS if length % p == 0)
    for p in range(parts):
        part = pl.ds(p * length // parts, length // parts)
        for n in range(count):
            pltpu.make_async_copy(refs[n].at[part], refs[count + n].at[part], sem.at[n]).start()
    for n in range(count):
        pltpu.make_async_copy(refs[n], refs[count + n], sem.at[n]).wait()


def stored(*arrays):
    inside = pl.BlockSpec(memory_space=pltpu.VMEM)
    return pl.pallas_call(
        store,
        out_shape=tuple(pltpu.HBM(x.shape, x.dtype) for x in arrays),
        in_specs=[inside] * len(arrays),
        out_specs=(pl.BlockSpec(memory_space=pltpu.HBM),) * len(arrays),
        scratch_shapes=[pltpu.SemaphoreType.DMA((len(arrays),))],
        compiler_params=pltpu.CompilerParams(vmem_limit_bytes=2**20),
    )(*(pltpu.with_memory_space_constraint(x, pltpu.VMEM) for x in arrays))


def by_kernel(nz, nw, grad, moment, weight):
    total, rows, cols = grad.shape
    side, mats = nz * rows, total // nz
    chunks = next(c for c in CHUNKS if mats % c == 0)
    dma = pltpu.SemaphoreType.DMA
    anywhere = pl.BlockSpec(memory_space=pl.ANY)
    shape = pltpu.VMEM(grad.shape, jnp.float32)
    local = pltpu.VMEM((total, rows, cols), jnp.float32)
    shared = pltpu.VMEM((nz, mats, rows, cols), jnp.float32)
    results = pl.pallas_call(
        functools.partial(kernel, nz, nw, chunks, mats // chunks),
        out_shape=(shape, shape),
        in_specs=[anywhere] * 3,
        out_specs=(pl.BlockSpec(memory_space=pltpu.VMEM),) * 2,
        scratch_shapes=[
            local, local, local,
            shared,
            pltpu.VMEM((nw, mats, side, side), jnp.float32),
            shared,
            local,
            dma((3,)),
            dma((1,)), dma((chunks,)),
            dma((chunks,)), dma((2,)),
            pltpu.SemaphoreType.REGULAR, pltpu.SemaphoreType.REGULAR,
        ],
        compiler_params=pltpu.CompilerParams(
            collective_id=0, has_side_effects=True, vmem_limit_bytes=40 * 2**20),
    )(*(pltpu.with_memory_space_constraint(x, pltpu.HBM) for x in (grad, moment, weight)))
    return stored(*results)


def by_ops(new_momentum):
    moved = lax.all_to_all(new_momentum, "zero", split_axis=0, concat_axis=1, tiled=True)
    gram = jnp.einsum("mik,mjk->mij", moved, moved, precision=lax.Precision.HIGHEST)
    gram = lax.psum(gram, "width")
    eye = jnp.eye(gram.shape[1], dtype=jnp.float32)
    scale = lax.rsqrt(jnp.sum(gram * eye, axis=(1, 2), keepdims=True) + 1e-06)
    gram = gram * (scale * scale)
    dot = functools.partial(jnp.einsum, "mij,mjk->mik", precision=lax.Precision.HIGHEST)
    held = None
    for step in range(ITERS):
        mixed = 3.4445 * eye - 4.775 * gram + 2.0315 * dot(gram, gram)
        held = mixed if held is None else dot(mixed, held)
        gram = dot(dot(mixed, gram), mixed)
    out = dot(held * scale, moved)
    return lax.all_to_all(out, "zero", split_axis=1, concat_axis=0, tiled=True)


def body(nz, nw, grad_stack, moment_stack, weight_stack):
    if grad_stack.shape[1] % 8 == 0 and nz & (nz - 1) == 0 and nz > 2:
        return by_kernel(nz, nw, grad_stack, moment_stack, weight_stack)
    new_momentum = hold_rate * moment_stack + grad_stack
    new_weights = keep_rate * weight_stack - learn_rate * by_ops(new_momentum)
    return (new_weights, new_momentum)


def solution(mesh):
    return jax.shard_map(
        functools.partial(body, mesh.shape["zero"], mesh.shape["width"]),
        mesh=mesh,
        in_specs=(
            P("unit", "zero", "width"),
            P("unit", "zero", "width"),
            P("unit", "zero", "width"),
        ),
        out_specs=(P("unit", "zero", "width"), P("unit", "zero", "width")),
        check_vma=False,
    )
```

```python
import functools

import jax
import jax.numpy as jnp
from jax import lax
from jax.experimental import pallas as pl
from jax.experimental.pallas import tpu as pltpu
from jax.sharding import PartitionSpec as P

ITERS = 3
GATHER_FROM = 1
RESULT_FROM = 1
CHUNKS = (4, 2, 1)
PARTS = (32, 16, 8, 4, 2, 1)
AHEAD = 3
PLAN = 2
MESH = pl.DeviceIdType.MESH


hold_rate = 0.95
learn_rate = 0.8
decay_rate = 0.1
keep_rate = 1.0 - learn_rate * decay_rate


def split(value):
    high = value.astype(jnp.bfloat16)
    low = (value - high.astype(jnp.float32)).astype(jnp.bfloat16)
    return high, low


def product(left, right, over):
    dims = (((1,), (over,)), ((), ()))
    dot = functools.partial(lax.dot_general, dimension_numbers=dims, preferred_element_type=jnp.float32)
    (lh, ll), (rh, rl) = left, right
    return dot(lh, rh) + (dot(lh, rl) + dot(ll, rh))


def orders(count):
    near = list(range(1, count))
    return near[GATHER_FROM:] + near[:GATHER_FROM], near[RESULT_FROM:] + near[:RESULT_FROM]


def paired(index, d, count):
    if d == 0:
        return index
    out, bit = 0, 1
    while bit < count:
        out = out + bit * ((index // bit + d // bit) % 2)
        bit *= 2
    return out


def factor(gram):
    side = gram.shape[0]
    rows = lax.broadcasted_iota(jnp.int32, (side, side), 0)
    cols = lax.broadcasted_iota(jnp.int32, (side, side), 1)
    eye = jnp.where(rows == cols, 1.0, 0.0).astype(jnp.float32)
    total = jnp.sum(jnp.sum(gram * eye, axis=1, keepdims=True), axis=0, keepdims=True)
    scale = lax.rsqrt(total + 1e-06)
    gram = gram * (scale * scale)
    held = None
    for step in range(ITERS):
        gs = split(gram)
        mixed = 3.4445 * eye - 4.775 * gram + 2.0315 * product(gs, gs, 0)
        ms = split(mixed)
        held = mixed if held is None else product(ms, split(held), 0)
        if step < ITERS - 1:
            gram = product(split(product(ms, gs, 0)), ms, 0)
    return held * scale


def kernel(nz, nw, chunks, per, grad, moment, weight, new_weights, new_momentum,
           grads, moments, weights, gather, grams, result, back,
           l_sem, g_send, g_recv, p_recv, r_recv, column, all_in):
    zi, wi = lax.axis_index("zero"), lax.axis_index("width")
    mats = chunks * per
    rows, cols = grad.shape[1], grad.shape[2]
    side = nz * rows
    gather_order, result_order = orders(nz)
    ahead = min(AHEAD, chunks)
    far = nz - 1
    pieces = [(far, k) for k in range(ahead)]
    pieces += [(d, k) for k in range(ahead) for d in gather_order if d != far]
    pieces += [(d, k) for k in range(ahead, chunks) for d in gather_order]
    pieces += [(0, k) for k in range(chunks)]
    inners = (nz // 2 - 1, nz // 2)
    outers = [z for z in range(nz) if z not in inners]
    inner = (zi == inners[0]) | (zi == inners[1])
    outer = jnp.logical_not(inner)

    def partner(d):
        return paired(zi, d, nz)

    barrier = pltpu.get_barrier_semaphore()

    def tell(sem, axis, index):
        pl.semaphore_signal(sem, inc=1, device_id={axis: index}, device_id_type=MESH)

    def piece(d, k):
        return pl.ds(partner(d) * mats + k * per, per)

    def group(n):
        return 0 if n == 0 else 1 + 2 * n // len(pieces)

    def load(which, n):
        source, target = ((grad, grads), (moment, moments))[which]
        return pltpu.make_async_copy(source.at[piece(*pieces[n])], target.at[piece(*pieces[n])], l_sem.at[group(n)])

    def load_weight():
        return pltpu.make_async_copy(weight, weights, l_sem.at[0])

    def wait_all(sem, *refs):
        for ref in refs:
            pltpu.make_async_copy(ref, ref, sem).wait()

    def gather_copy(d, k):
        return pltpu.make_async_remote_copy(
            src_ref=new_momentum.at[piece(d, k)],
            dst_ref=gather.at[zi, pl.ds(k * per, per)],
            send_sem=g_send.at[0], recv_sem=g_recv.at[k],
            device_id={"zero": partner(d)}, device_id_type=MESH)

    def gram_copy(d, k):
        return pltpu.make_async_remote_copy(
            src_ref=grams.at[wi, pl.ds(k * per, per)],
            dst_ref=grams.at[wi, pl.ds(k * per, per)],
            send_sem=l_sem.at[1], recv_sem=p_recv.at[k],
            device_id={"width": lax.rem(wi + d, nw)}, device_id_type=MESH)

    def result_copy(d, k):
        return pltpu.make_async_remote_copy(
            src_ref=result.at[partner(d), pl.ds(k * per, per)],
            dst_ref=back.at[piece(0, k)],
            send_sem=l_sem.at[2], recv_sem=r_recv.at[(1 + int(d == far)) * int(k == chunks - 1)],
            device_id={"zero": partner(d)}, device_id_type=MESH)

    @pl.when(inner)
    def _():
        tell(barrier, "zero", partner(far))

    for i in range(per):
        for row in range(0, rows, 8):
            for source, target in ((grad, grads), (moment, moments)):
                part = (partner(far) * mats + i, pl.ds(row, 8))
                pltpu.make_async_copy(source.at[part], target.at[part], l_sem.at[0]).start()
    for z in outers:
        @pl.when(zi != z)
        def _():
            tell(barrier, "zero", z)

    @pl.when(outer)
    def _():
        for d in range(1, nw):
            tell(barrier, "width", lax.rem(wi + d, nw))

    for n in range(1, len(pieces)):
        load(0, n).start()
        load(1, n).start()

    def momentum(n):
        d, k = pieces[n]
        if n == 0 or group(n) != group(n - 1):
            members = sum(group(m) == group(n) for m in range(len(pieces)))
            wait_all(l_sem.at[group(n)], grads.at[pl.ds(0, 2 * members * per)])
        value = hold_rate * moments[piece(d, k)] + grads[piece(d, k)]
        new_momentum[piece(d, k)] = value
        if d == 0:
            gather[zi, pl.ds(k * per, per)] = value

    def release(d, k):
        if d:
            gather_copy(d, k).start()

    for n in range(len(pieces)):
        momentum(n)
        if n == 0:
            pl.semaphore_wait(barrier, jnp.where(inner, 1, nz + nw - 2))
            release(*pieces[0])

            @pl.when(outer)
            def _():
                for z in inners:
                    tell(column, "zero", z)
                for d in range(1, nw):
                    tell(all_in, "width", lax.rem(wi + d, nw))
        if n == ahead + 1:
            @pl.when(inner)
            def _():
                pl.semaphore_wait(column, len(outers))
        if n > 1:
            release(*pieces[n - 1])
    release(*pieces[-1])
    load_weight().start()

    @pl.when(outer)
    def _():
        pl.semaphore_wait(all_in, nw - 1)
        for z in inners:
            tell(all_in, "zero", z)

    def whole(i):
        return split(gather[:, i].reshape(side, cols))

    def finish(k):
        wait_all(p_recv.at[k], grams.at[pl.ds(0, nw - 1), pl.ds(k * per, per)])

        def one(j, carry):
            i = k * per + j
            gram = grams[0, i]
            for w in range(1, nw):
                gram = gram + grams[w, i]
            out = product(split(factor(gram)), whole(i), 0)
            result[:, i] = out.reshape(nz, rows, cols)
            return carry

        lax.fori_loop(0, per, one, 0)
        results = [(d, k) for d in result_order if d != far]
        if k > 0:
            results.insert(1, (far, k - 1))
        if k == chunks - 1:
            results.append((far, k))
        for piece_of in results:
            result_copy(*piece_of).start()

    def begin(k):
        wait_all(g_recv.at[k], gather.at[pl.ds(0, nz - 1), pl.ds(k * per, per)])

        def make(j, carry):
            i = k * per + j
            x = whole(i)
            grams[wi, i] = product(x, x, 1)
            return carry

        lax.fori_loop(0, per, make, 0)
        if k == 0:
            @pl.when(inner)
            def _():
                pl.semaphore_wait(all_in, len(outers))
        for d in range(1, nw):
            gram_copy(d, k).start()

    for k in range(min(PLAN, chunks)):
        begin(k)
    for k in range(min(PLAN, chunks)):
        finish(k)
    for k in range(min(PLAN, chunks), chunks):
        begin(k)
        finish(k)

    load_weight().wait()
    for k in range(chunks):
        new_weights[piece(0, k)] = keep_rate * weights[piece(0, k)] - learn_rate * result[zi, pl.ds(k * per, per)]
    wait_all(g_send.at[0], gather.at[pl.ds(0, nz - 1)])
    wait_all(l_sem.at[1], grams.at[pl.ds(0, nw - 1)])
    last = chunks - 1
    batches = [[(d, k) for k in range(last) for d in result_order], [(d, last) for d in result_order if d != far], [(far, last)]]
    for part, members in enumerate(batches):
        if members:
            wait_all(r_recv.at[part], back.at[pl.ds(0, per * len(members))])
        for d, k in members:
            new_weights[piece(d, k)] = keep_rate * weights[piece(d, k)] - learn_rate * back[piece(d, k)]

    wait_all(l_sem.at[2], result.at[pl.ds(0, nz - 1)])


def store(*refs):
    count = len(refs) // 2
    sem = refs[-1]
    length = refs[0].shape[0]
    parts = next(p for p in PARTS if length % p == 0)
    for p in range(parts):
        part = pl.ds(p * length // parts, length // parts)
        for n in range(count):
            pltpu.make_async_copy(refs[n].at[part], refs[count + n].at[part], sem.at[n]).start()
    for n in range(count):
        pltpu.make_async_copy(refs[n], refs[count + n], sem.at[n]).wait()


def stored(*arrays):
    inside = pl.BlockSpec(memory_space=pltpu.VMEM)
    return pl.pallas_call(
        store,
        out_shape=tuple(pltpu.HBM(x.shape, x.dtype) for x in arrays),
        in_specs=[inside] * len(arrays),
        out_specs=(pl.BlockSpec(memory_space=pltpu.HBM),) * len(arrays),
        scratch_shapes=[pltpu.SemaphoreType.DMA((len(arrays),))],
        compiler_params=pltpu.CompilerParams(vmem_limit_bytes=2**20),
    )(*(pltpu.with_memory_space_constraint(x, pltpu.VMEM) for x in arrays))


def by_kernel(nz, nw, grad, moment, weight):
    total, rows, cols = grad.shape
    side, mats = nz * rows, total // nz
    chunks = next(c for c in CHUNKS if mats % c == 0)
    dma = pltpu.SemaphoreType.DMA
    anywhere = pl.BlockSpec(memory_space=pl.ANY)
    shape = pltpu.VMEM(grad.shape, jnp.float32)
    local = pltpu.VMEM((total, rows, cols), jnp.float32)
    shared = pltpu.VMEM((nz, mats, rows, cols), jnp.float32)
    results = pl.pallas_call(
        functools.partial(kernel, nz, nw, chunks, mats // chunks),
        out_shape=(shape, shape),
        in_specs=[anywhere] * 3,
        out_specs=(pl.BlockSpec(memory_space=pltpu.VMEM),) * 2,
        scratch_shapes=[
            local, local, local,
            shared,
            pltpu.VMEM((nw, mats, side, side), jnp.float32),
            shared,
            local,
            dma((3,)),
            dma((1,)), dma((chunks,)),
            dma((chunks,)), dma((3,)),
            pltpu.SemaphoreType.REGULAR, pltpu.SemaphoreType.REGULAR,
        ],
        compiler_params=pltpu.CompilerParams(
            collective_id=0, has_side_effects=True, vmem_limit_bytes=40 * 2**20),
    )(*(pltpu.with_memory_space_constraint(x, pltpu.HBM) for x in (grad, moment, weight)))
    return stored(*results)


def by_ops(new_momentum):
    moved = lax.all_to_all(new_momentum, "zero", split_axis=0, concat_axis=1, tiled=True)
    gram = jnp.einsum("mik,mjk->mij", moved, moved, precision=lax.Precision.HIGHEST)
    gram = lax.psum(gram, "width")
    eye = jnp.eye(gram.shape[1], dtype=jnp.float32)
    scale = lax.rsqrt(jnp.sum(gram * eye, axis=(1, 2), keepdims=True) + 1e-06)
    gram = gram * (scale * scale)
    dot = functools.partial(jnp.einsum, "mij,mjk->mik", precision=lax.Precision.HIGHEST)
    held = None
    for step in range(ITERS):
        mixed = 3.4445 * eye - 4.775 * gram + 2.0315 * dot(gram, gram)
        held = mixed if held is None else dot(mixed, held)
        gram = dot(dot(mixed, gram), mixed)
    out = dot(held * scale, moved)
    return lax.all_to_all(out, "zero", split_axis=1, concat_axis=0, tiled=True)


def body(nz, nw, grad_stack, moment_stack, weight_stack):
    if grad_stack.shape[1] % 8 == 0 and nz & (nz - 1) == 0 and nz > 2:
        return by_kernel(nz, nw, grad_stack, moment_stack, weight_stack)
    new_momentum = hold_rate * moment_stack + grad_stack
    new_weights = keep_rate * weight_stack - learn_rate * by_ops(new_momentum)
    return (new_weights, new_momentum)


def solution(mesh):
    return jax.shard_map(
        functools.partial(body, mesh.shape["zero"], mesh.shape["width"]),
        mesh=mesh,
        in_specs=(
            P("unit", "zero", "width"),
            P("unit", "zero", "width"),
            P("unit", "zero", "width"),
        ),
        out_specs=(P("unit", "zero", "width"), P("unit", "zero", "width")),
        check_vma=False,
    )
```

```python
import functools

import jax
import jax.numpy as jnp
from jax import lax
from jax.experimental import pallas as pl
from jax.experimental.pallas import tpu as pltpu
from jax.sharding import PartitionSpec as P

ITERS = 3
GATHER_FROM = 1
RESULT_FROM = 1
CHUNKS = (4, 2, 1)
PARTS = (32, 16, 8, 4, 2, 1)
AHEAD = 4
PLAN = 2
MESH = pl.DeviceIdType.MESH


hold_rate = 0.95
learn_rate = 0.8
decay_rate = 0.1
keep_rate = 1.0 - learn_rate * decay_rate


def split(value):
    high = value.astype(jnp.bfloat16)
    low = (value - high.astype(jnp.float32)).astype(jnp.bfloat16)
    return high, low


def product(left, right, over):
    dims = (((1,), (over,)), ((), ()))
    dot = functools.partial(lax.dot_general, dimension_numbers=dims, preferred_element_type=jnp.float32)
    (lh, ll), (rh, rl) = left, right
    return dot(lh, rh) + (dot(lh, rl) + dot(ll, rh))


def orders(count):
    near = list(range(1, count))
    return near[GATHER_FROM:] + near[:GATHER_FROM], near[RESULT_FROM:] + near[:RESULT_FROM]


def paired(index, d, count):
    if d == 0:
        return index
    out, bit = 0, 1
    while bit < count:
        out = out + bit * ((index // bit + d // bit) % 2)
        bit *= 2
    return out


def factor(gram):
    side = gram.shape[0]
    rows = lax.broadcasted_iota(jnp.int32, (side, side), 0)
    cols = lax.broadcasted_iota(jnp.int32, (side, side), 1)
    eye = jnp.where(rows == cols, 1.0, 0.0).astype(jnp.float32)
    total = jnp.sum(jnp.sum(gram * eye, axis=1, keepdims=True), axis=0, keepdims=True)
    scale = lax.rsqrt(total + 1e-06)
    gram = gram * (scale * scale)
    held = None
    for step in range(ITERS):
        gs = split(gram)
        mixed = 3.4445 * eye - 4.775 * gram + 2.0315 * product(gs, gs, 0)
        ms = split(mixed)
        held = mixed if held is None else product(ms, split(held), 0)
        if step < ITERS - 1:
            gram = product(split(product(ms, gs, 0)), ms, 0)
    return held * scale


def kernel(nz, nw, chunks, per, grad, moment, weight, new_weights, new_momentum,
           grads, moments, weights, gather, grams, result, back,
           l_sem, g_send, g_recv, p_recv, r_recv, column, all_in):
    zi, wi = lax.axis_index("zero"), lax.axis_index("width")
    mats = chunks * per
    rows, cols = grad.shape[1], grad.shape[2]
    side = nz * rows
    gather_order, result_order = orders(nz)
    ahead = min(AHEAD, chunks)
    far = nz - 1
    pieces = [(far, k) for k in range(ahead)]
    pieces += [(d, k) for k in range(ahead) for d in gather_order if d != far]
    pieces += [(d, k) for k in range(ahead, chunks) for d in gather_order]
    pieces += [(0, k) for k in range(chunks)]
    inners = (nz // 2 - 1, nz // 2)
    outers = [z for z in range(nz) if z not in inners]
    inner = (zi == inners[0]) | (zi == inners[1])
    outer = jnp.logical_not(inner)

    def partner(d):
        return paired(zi, d, nz)

    barrier = pltpu.get_barrier_semaphore()

    def tell(sem, axis, index):
        pl.semaphore_signal(sem, inc=1, device_id={axis: index}, device_id_type=MESH)

    def piece(d, k):
        return pl.ds(partner(d) * mats + k * per, per)

    def group(n):
        return 0 if n == 0 else 1 + 2 * n // len(pieces)

    def load(which, n):
        source, target = ((grad, grads), (moment, moments))[which]
        return pltpu.make_async_copy(source.at[piece(*pieces[n])], target.at[piece(*pieces[n])], l_sem.at[group(n)])

    def load_weight():
        return pltpu.make_async_copy(weight, weights, l_sem.at[0])

    def wait_all(sem, *refs):
        for ref in refs:
            pltpu.make_async_copy(ref, ref, sem).wait()

    def gather_copy(d, k):
        return pltpu.make_async_remote_copy(
            src_ref=new_momentum.at[piece(d, k)],
            dst_ref=gather.at[zi, pl.ds(k * per, per)],
            send_sem=g_send.at[0], recv_sem=g_recv.at[k],
            device_id={"zero": partner(d)}, device_id_type=MESH)

    def gram_copy(d, k):
        return pltpu.make_async_remote_copy(
            src_ref=grams.at[wi, pl.ds(k * per, per)],
            dst_ref=grams.at[wi, pl.ds(k * per, per)],
            send_sem=l_sem.at[1], recv_sem=p_recv.at[k],
            device_id={"width": lax.rem(wi + d, nw)}, device_id_type=MESH)

    def result_copy(d, k):
        return pltpu.make_async_remote_copy(
            src_ref=result.at[partner(d), pl.ds(k * per, per)],
            dst_ref=back.at[piece(0, k)],
            send_sem=l_sem.at[2], recv_sem=r_recv.at[(1 + int(d == far)) * int(k == chunks - 1)],
            device_id={"zero": partner(d)}, device_id_type=MESH)

    @pl.when(inner)
    def _():
        tell(barrier, "zero", partner(far))

    for i in range(per):
        for row in range(0, rows, 8):
            for source, target in ((grad, grads), (moment, moments)):
                part = (partner(far) * mats + i, pl.ds(row, 8))
                pltpu.make_async_copy(source.at[part], target.at[part], l_sem.at[0]).start()
    for z in outers:
        @pl.when(zi != z)
        def _():
            tell(barrier, "zero", z)

    @pl.when(outer)
    def _():
        for d in range(1, nw):
            tell(barrier, "width", lax.rem(wi + d, nw))

    for n in range(1, len(pieces)):
        load(0, n).start()
        load(1, n).start()

    def momentum(n):
        d, k = pieces[n]
        if n == 0 or group(n) != group(n - 1):
            members = sum(group(m) == group(n) for m in range(len(pieces)))
            wait_all(l_sem.at[group(n)], grads.at[pl.ds(0, 2 * members * per)])
        value = hold_rate * moments[piece(d, k)] + grads[piece(d, k)]
        new_momentum[piece(d, k)] = value
        if d == 0:
            gather[zi, pl.ds(k * per, per)] = value

    def release(d, k):
        if d:
            gather_copy(d, k).start()

    for n in range(len(pieces)):
        momentum(n)
        if n == 0:
            pl.semaphore_wait(barrier, jnp.where(inner, 1, nz + nw - 2))
            release(*pieces[0])

            @pl.when(outer)
            def _():
                for z in inners:
                    tell(column, "zero", z)
                for d in range(1, nw):
                    tell(all_in, "width", lax.rem(wi + d, nw))
        if n == ahead + 1:
            @pl.when(inner)
            def _():
                pl.semaphore_wait(column, len(outers))
        if n > 1:
            release(*pieces[n - 1])
    release(*pieces[-1])
    load_weight().start()

    @pl.when(outer)
    def _():
        pl.semaphore_wait(all_in, nw - 1)
        for z in inners:
            tell(all_in, "zero", z)

    def whole(i):
        return split(gather[:, i].reshape(side, cols))

    def finish(k):
        wait_all(p_recv.at[k], grams.at[pl.ds(0, nw - 1), pl.ds(k * per, per)])

        def one(j, carry):
            i = k * per + j
            gram = grams[0, i]
            for w in range(1, nw):
                gram = gram + grams[w, i]
            out = product(split(factor(gram)), whole(i), 0)
            result[:, i] = out.reshape(nz, rows, cols)
            return carry

        lax.fori_loop(0, per, one, 0)
        results = [(d, k) for d in result_order if d != far]
        if k > 0:
            results.insert(1, (far, k - 1))
        if k == chunks - 1:
            results.append((far, k))
        for piece_of in results:
            result_copy(*piece_of).start()

    def begin(k):
        wait_all(g_recv.at[k], gather.at[pl.ds(0, nz - 1), pl.ds(k * per, per)])

        def make(j, carry):
            i = k * per + j
            x = whole(i)
            grams[wi, i] = product(x, x, 1)
            return carry

        lax.fori_loop(0, per, make, 0)
        if k == 0:
            @pl.when(inner)
            def _():
                pl.semaphore_wait(all_in, len(outers))
        for d in range(1, nw):
            gram_copy(d, k).start()

    for k in range(min(PLAN, chunks)):
        begin(k)
    for k in range(min(PLAN, chunks)):
        finish(k)
    for k in range(min(PLAN, chunks), chunks):
        begin(k)
        finish(k)

    load_weight().wait()
    for k in range(chunks):
        new_weights[piece(0, k)] = keep_rate * weights[piece(0, k)] - learn_rate * result[zi, pl.ds(k * per, per)]
    wait_all(g_send.at[0], gather.at[pl.ds(0, nz - 1)])
    wait_all(l_sem.at[1], grams.at[pl.ds(0, nw - 1)])
    last = chunks - 1
    batches = [[(d, k) for k in range(last) for d in result_order], [(d, last) for d in result_order if d != far], [(far, last)]]
    for part, members in enumerate(batches):
        if members:
            wait_all(r_recv.at[part], back.at[pl.ds(0, per * len(members))])
        for d, k in members:
            new_weights[piece(d, k)] = keep_rate * weights[piece(d, k)] - learn_rate * back[piece(d, k)]

    wait_all(l_sem.at[2], result.at[pl.ds(0, nz - 1)])


def store(*refs):
    count = len(refs) // 2
    sem = refs[-1]
    length = refs[0].shape[0]
    parts = next(p for p in PARTS if length % p == 0)
    for p in range(parts):
        part = pl.ds(p * length // parts, length // parts)
        for n in range(count):
            pltpu.make_async_copy(refs[n].at[part], refs[count + n].at[part], sem.at[n]).start()
    for n in range(count):
        pltpu.make_async_copy(refs[n], refs[count + n], sem.at[n]).wait()


def stored(*arrays):
    inside = pl.BlockSpec(memory_space=pltpu.VMEM)
    return pl.pallas_call(
        store,
        out_shape=tuple(pltpu.HBM(x.shape, x.dtype) for x in arrays),
        in_specs=[inside] * len(arrays),
        out_specs=(pl.BlockSpec(memory_space=pltpu.HBM),) * len(arrays),
        scratch_shapes=[pltpu.SemaphoreType.DMA((len(arrays),))],
        compiler_params=pltpu.CompilerParams(vmem_limit_bytes=2**20),
    )(*(pltpu.with_memory_space_constraint(x, pltpu.VMEM) for x in arrays))


def by_kernel(nz, nw, grad, moment, weight):
    total, rows, cols = grad.shape
    side, mats = nz * rows, total // nz
    chunks = next(c for c in CHUNKS if mats % c == 0)
    dma = pltpu.SemaphoreType.DMA
    anywhere = pl.BlockSpec(memory_space=pl.ANY)
    shape = pltpu.VMEM(grad.shape, jnp.float32)
    local = pltpu.VMEM((total, rows, cols), jnp.float32)
    shared = pltpu.VMEM((nz, mats, rows, cols), jnp.float32)
    results = pl.pallas_call(
        functools.partial(kernel, nz, nw, chunks, mats // chunks),
        out_shape=(shape, shape),
        in_specs=[anywhere] * 3,
        out_specs=(pl.BlockSpec(memory_space=pltpu.VMEM),) * 2,
        scratch_shapes=[
            local, local, local,
            shared,
            pltpu.VMEM((nw, mats, side, side), jnp.float32),
            shared,
            local,
            dma((3,)),
            dma((1,)), dma((chunks,)),
            dma((chunks,)), dma((3,)),
            pltpu.SemaphoreType.REGULAR, pltpu.SemaphoreType.REGULAR,
        ],
        compiler_params=pltpu.CompilerParams(
            collective_id=0, has_side_effects=True, vmem_limit_bytes=40 * 2**20),
    )(*(pltpu.with_memory_space_constraint(x, pltpu.HBM) for x in (grad, moment, weight)))
    return stored(*results)


def by_ops(new_momentum):
    moved = lax.all_to_all(new_momentum, "zero", split_axis=0, concat_axis=1, tiled=True)
    gram = jnp.einsum("mik,mjk->mij", moved, moved, precision=lax.Precision.HIGHEST)
    gram = lax.psum(gram, "width")
    eye = jnp.eye(gram.shape[1], dtype=jnp.float32)
    scale = lax.rsqrt(jnp.sum(gram * eye, axis=(1, 2), keepdims=True) + 1e-06)
    gram = gram * (scale * scale)
    dot = functools.partial(jnp.einsum, "mij,mjk->mik", precision=lax.Precision.HIGHEST)
    held = None
    for step in range(ITERS):
        mixed = 3.4445 * eye - 4.775 * gram + 2.0315 * dot(gram, gram)
        held = mixed if held is None else dot(mixed, held)
        gram = dot(dot(mixed, gram), mixed)
    out = dot(held * scale, moved)
    return lax.all_to_all(out, "zero", split_axis=1, concat_axis=0, tiled=True)


def body(nz, nw, grad_stack, moment_stack, weight_stack):
    if grad_stack.shape[1] % 8 == 0 and nz & (nz - 1) == 0 and nz > 2:
        return by_kernel(nz, nw, grad_stack, moment_stack, weight_stack)
    new_momentum = hold_rate * moment_stack + grad_stack
    new_weights = keep_rate * weight_stack - learn_rate * by_ops(new_momentum)
    return (new_weights, new_momentum)


def solution(mesh):
    return jax.shard_map(
        functools.partial(body, mesh.shape["zero"], mesh.shape["width"]),
        mesh=mesh,
        in_specs=(
            P("unit", "zero", "width"),
            P("unit", "zero", "width"),
            P("unit", "zero", "width"),
        ),
        out_specs=(P("unit", "zero", "width"), P("unit", "zero", "width")),
        check_vma=False,
    )
```
